8 devices in a mesh: rep: 1 (over z), ep: 8 (over y, x, core).
Axes of the slice: x: 2, y: 2, z: 1, core: 2. Of those that a mesh axis runs over, the one named last changes fastest.
Arguments:
- x: bfloat16 [1024, 2048], P(('rep', 'ep'))
- cache: bfloat16 [1024, 256, 576], P(('rep', 'ep'))
- lens: int32 [1024], P(('rep', 'ep'))
- ids: int32 [1024, 6], P(('rep', 'ep'))
- rw: float32 [1024, 6], P(('rep', 'ep'))
- w_q: bfloat16 [2048, 3072], replicated
- w_dkv: bfloat16 [2048, 576], replicated
- w_uk: bfloat16 [16, 128, 512], replicated
- w_uv: bfloat16 [16, 512, 128], replicated
- w_o: bfloat16 [2048, 2048], replicated
- s_gate: bfloat16 [2048, 2816], replicated
- s_up: bfloat16 [2048, 2816], replicated
- s_down: bfloat16 [2816, 2048], replicated
- e_gate: bfloat16 [64, 2048, 1408], P('ep')
- e_up: bfloat16 [64, 2048, 1408], P('ep')
- e_down: bfloat16 [64, 1408, 2048], P('ep')
Outputs:
- output 1: bfloat16 [1024, 2048], P(('rep', 'ep'))
- output 2: bfloat16 [1024, 576], P(('rep', 'ep'))
All inputs are finite; a program needn't handle non-finite values.
Results may differ from the reference program's by a relative error of at most 0.0118949.
Values are sent between devices in bfloat16 or wider.
A program may use at most 1 GiB of HBM per device.

```python
import jax
import jax.numpy as jnp
from jax import lax

EP = 8
B_DEV = 128
L_MAX = 256
H = 2048
HEADS = 16
KV_LORA = 512
ROPE = 64
NOPE = 128
VHEAD = 128
EXPERTS = 64
TOP = 6
INTER = 1408
SHARED = 2816

B = EP * B_DEV
KVD = KV_LORA + ROPE
QKD = NOPE + ROPE
LEN_LO = (3 * L_MAX) // 4
EPS = 1e-6
ROPE_BASE = 1.0e4


def rms(v):
    v = v.astype(jnp.float32)
    return v * lax.rsqrt(jnp.mean(v * v, axis=-1, keepdims=True) + EPS)


def rope(v, pos):
    half = v.shape[-1] // 2
    inv = ROPE_BASE ** (-2.0 * jnp.arange(half, dtype=jnp.float32) / v.shape[-1])
    ang = pos.astype(jnp.float32)[..., None] * inv
    cs = jnp.cos(ang)
    sn = jnp.sin(ang)
    v1 = v[..., :half]
    v2 = v[..., half:]
    return jnp.concatenate([v1 * cs - v2 * sn, v2 * cs + v1 * sn], axis=-1)


def swiglu(u, wg, wu, wd):
    g = jnp.dot(u, wg, preferred_element_type=jnp.float32)
    v = jnp.dot(u, wu, preferred_element_type=jnp.float32)
    return jnp.dot((jax.nn.silu(g) * v).astype(jnp.bfloat16), wd, preferred_element_type=jnp.float32)


def setup_inputs(seed: int = 0, part: int = 0) -> dict:
    kbase = jax.random.fold_in(jax.random.key(seed), part)
    kp = jax.random.split(kbase, 8)
    kd = jax.random.split(jax.random.fold_in(kbase, 7), 3)
    kw = jax.random.split(jax.random.key(seed + 1), 11)

    def draw(k, shape, fan):
        return (jax.random.normal(k, shape, jnp.float32) * fan ** -0.5).astype(jnp.bfloat16)

    x = jax.random.normal(kp[0], (B, H), jnp.float32).astype(jnp.bfloat16)
    span = (L_MAX - LEN_LO) // 8
    dev = jnp.arange(B) // B_DEV
    low = jax.random.randint(kd[0], (B,), LEN_LO, LEN_LO + span)
    high = jax.random.randint(kd[1], (B,), L_MAX - span, L_MAX)
    lens = jnp.where(dev % 2 == 0, low, high).astype(jnp.int32)
    pos = jnp.arange(L_MAX)[None, :, None]
    m_live = 0.7 * jax.random.normal(kp[2], (B, 1, KVD), jnp.float32)
    m_old = 0.7 * jax.random.normal(kp[3], (B, 1, KVD), jnp.float32)
    noise = jax.random.normal(kp[4], (B, L_MAX, KVD), jnp.float32)
    cache = (jnp.where(pos < lens[:, None, None], m_live, m_old) + noise).astype(jnp.bfloat16)

    def route(k):
        k1, k2 = jax.random.split(k)
        perm_e = jax.random.permutation(k1, EXPERTS)
        perm_t = jax.random.permutation(k2, B_DEV)
        j = jnp.arange(B_DEV)[:, None] * TOP + jnp.arange(TOP)[None, :]
        return perm_e[j % (EXPERTS // 2)][perm_t]

    ids = jax.vmap(route)(jax.random.split(kd[2], EP)).reshape(B, TOP).astype(jnp.int32)
    rw = jax.random.uniform(kp[6], (B, TOP), jnp.float32, 0.5, 1.5) * TOP ** -0.5
    return {
        'x': x,
        'cache': cache,
        'lens': lens,
        'ids': ids,
        'rw': rw,
        'w_q': draw(kw[0], (H, HEADS * QKD), H),
        'w_dkv': draw(kw[1], (H, KVD), H),
        'w_uk': draw(kw[2], (HEADS, NOPE, KV_LORA), NOPE),
        'w_uv': draw(kw[3], (HEADS, KV_LORA, VHEAD), KV_LORA),
        'w_o': draw(kw[4], (HEADS * VHEAD, H), HEADS * VHEAD),
        's_gate': draw(kw[5], (H, SHARED), H),
        's_up': draw(kw[6], (H, SHARED), H),
        's_down': draw(kw[7], (SHARED, H), SHARED),
        'e_gate': draw(kw[8], (EXPERTS, H, INTER), H),
        'e_up': draw(kw[9], (EXPERTS, H, INTER), H),
        'e_down': draw(kw[10], (EXPERTS, INTER, H), INTER),
    }


def reference(x, cache, lens, ids, rw, w_q, w_dkv, w_uk, w_uv, w_o, s_gate, s_up, s_down, e_gate, e_up, e_down):
    xn = rms(x).astype(jnp.bfloat16)
    q = jnp.dot(xn, w_q, preferred_element_type=jnp.float32).astype(jnp.bfloat16).reshape(B, HEADS, QKD)
    kv = jnp.dot(xn, w_dkv, preferred_element_type=jnp.float32)
    kv_new = jnp.concatenate([rms(kv[:, :KV_LORA]), rope(kv[:, KV_LORA:], lens)], axis=-1).astype(jnp.bfloat16)
    q_lat = jnp.einsum('bhd,hdc->bhc', q[:, :, :NOPE].astype(jnp.float32), w_uk.astype(jnp.float32)).astype(jnp.bfloat16)
    q_rot = rope(q[:, :, NOPE:].astype(jnp.float32), lens[:, None]).astype(jnp.bfloat16)
    qf = jnp.concatenate([q_lat, q_rot], axis=-1)
    scale = QKD ** -0.5

    def attend(args):
        qb, cb, kb, lb = args
        qs = qb.astype(jnp.float32)
        cs = cb.astype(jnp.float32)
        ks = kb.astype(jnp.float32)
        s = jnp.dot(qs, cs.T) * scale
        s = jnp.where(jnp.arange(L_MAX)[None, :] < lb, s, -jnp.inf)
        s_new = jnp.dot(qs, ks) * scale
        mx = jnp.maximum(jnp.max(s, axis=1), s_new)
        e = jnp.exp(s - mx[:, None])
        e_new = jnp.exp(s_new - mx)
        den = jnp.sum(e, axis=1) + e_new
        p = (e / den[:, None]).astype(jnp.bfloat16).astype(jnp.float32)
        p_new = (e_new / den).astype(jnp.bfloat16).astype(jnp.float32)
        o = jnp.dot(p, cs[:, :KV_LORA]) + p_new[:, None] * ks[None, :KV_LORA]
        return o.astype(jnp.bfloat16)

    o_lat = lax.map(attend, (qf, cache, kv_new, lens))
    o = jnp.einsum('bhc,hcv->bhv', o_lat.astype(jnp.float32), w_uv.astype(jnp.float32)).astype(jnp.bfloat16).reshape(B, HEADS * VHEAD)
    a = jnp.dot(o, w_o, preferred_element_type=jnp.float32)
    h1 = (x.astype(jnp.float32) + a).astype(jnp.bfloat16)
    u = rms(h1).astype(jnp.bfloat16)
    shared = swiglu(u, s_gate, s_up, s_down)
    gate_w = jnp.sum(jnp.where(ids[:, :, None] == jnp.arange(EXPERTS)[None, None, :], rw[:, :, None], 0.0), axis=1)

    def expert(acc, args):
        wg, wu, wd, cw = args
        out = swiglu(u, wg, wu, wd).astype(jnp.bfloat16).astype(jnp.float32)
        return acc + cw[:, None] * out, None

    routed, _ = lax.scan(expert, jnp.zeros((B, H), jnp.float32), (e_gate, e_up, e_down, gate_w.T))
    y = (h1.astype(jnp.float32) + shared + routed).astype(jnp.bfloat16)
    return y, kv_new
```

```python
import jax
import jax.numpy as jnp
from jax import lax
from jax.experimental import pallas as pl
from jax.experimental.pallas import tpu as pltpu
from jax.sharding import PartitionSpec as P

EPS = 1e-6
ROPE_BASE = 1.0e4
BF = jnp.bfloat16
F32 = jnp.float32
CAP = 24
CW = 256


def rms(v):
    v = v.astype(jnp.float32)
    return v * lax.rsqrt(jnp.mean(v * v, axis=-1, keepdims=True) + EPS)


def rope(v, pos):
    half = v.shape[-1] // 2
    inv = ROPE_BASE ** (-2.0 * jnp.arange(half, dtype=jnp.float32) / v.shape[-1])
    ang = pos.astype(jnp.float32)[..., None] * inv
    cs = jnp.cos(ang)
    sn = jnp.sin(ang)
    v1 = v[..., :half]
    v2 = v[..., half:]
    return jnp.concatenate([v1 * cs - v2 * sn, v2 * cs + v1 * sn], axis=-1)


def attention(x, cache, lens, w_q, w_dkv, w_uk, w_uv, w_o):
    bsz = x.shape[0]
    heads, nope, kvl = w_uk.shape
    kvd = cache.shape[2]
    vh = w_uv.shape[2]
    qkd = nope + kvd - kvl
    xn = rms(x).astype(jnp.bfloat16)
    q = jnp.dot(xn, w_q, preferred_element_type=jnp.float32).astype(jnp.bfloat16).reshape(bsz, heads, qkd)
    kv = jnp.dot(xn, w_dkv, preferred_element_type=jnp.float32)
    kv_new = jnp.concatenate([rms(kv[:, :kvl]), rope(kv[:, kvl:], lens)], axis=-1).astype(jnp.bfloat16)
    q_lat = jnp.einsum('bhd,hdc->bhc', q[:, :, :nope], w_uk, preferred_element_type=jnp.float32).astype(jnp.bfloat16)
    q_rot = rope(q[:, :, nope:].astype(jnp.float32), lens[:, None]).astype(jnp.bfloat16)
    qf = jnp.concatenate([q_lat, q_rot], axis=-1)
    scale = qkd ** -0.5
    s = jnp.einsum('bhc,blc->bhl', qf, cache, preferred_element_type=jnp.float32) * scale
    live = jnp.arange(cache.shape[1])[None, None, :] < lens[:, None, None]
    s = jnp.where(live, s, -jnp.inf)
    s_new = jnp.einsum('bhc,bc->bh', qf, kv_new, preferred_element_type=jnp.float32) * scale
    mx = jnp.maximum(jnp.max(s, axis=2), s_new)
    e = jnp.exp(s - mx[:, :, None])
    e_new = jnp.exp(s_new - mx)
    den = jnp.sum(e, axis=2) + e_new
    p = (e / den[:, :, None]).astype(jnp.bfloat16)
    p_new = (e_new / den).astype(jnp.bfloat16)
    o_all = jnp.einsum('bhl,blc->bhc', p, cache, preferred_element_type=jnp.float32)
    o_lat = (o_all[:, :, :kvl] + p_new.astype(jnp.float32)[:, :, None] * kv_new[:, None, :kvl].astype(jnp.float32)).astype(jnp.bfloat16)
    o = jnp.einsum('bhc,hcv->bhv', o_lat, w_uv, preferred_element_type=jnp.float32).astype(jnp.bfloat16).reshape(bsz, heads * vh)
    a = jnp.dot(o, w_o, preferred_element_type=jnp.float32)
    return (x.astype(jnp.float32) + a).astype(jnp.bfloat16), kv_new


def moe_kernel(u_ref, h1_ref, wt_ref, sg, su, sd, eg, eu, ed, y_ref,
               u_all, wt_all, rank_s, wsel, pm, cm, xr, act, act_sh, orow, wa, wb, ybase,
               part, rx0, rx1, rx2, rx3, s1, keep0, s2, keep1, s3, keep2,
               sem_a, sem_b, wt_send, wt_recv, g_send, g_recv,
               d_send, d_recv):
    n = 8
    n_loc = 8
    hid = u_ref.shape[1]
    inter = wa.shape[2]
    nc = hid // CW
    me = lax.axis_index('ep')
    core = lax.rem(me, 2)
    chip = me // 2
    cx = lax.rem(chip, 2)
    cy = chip // 2
    sib = chip * 2 + 1 - core
    xn_ = (cy * 2 + 1 - cx) * 2 + core
    yn_ = ((1 - cy) * 2 + cx) * 2 + core
    dg = ((1 - cy) * 2 + 1 - cx) * 2 + core
    dev1 = xn_ * (1 - core) + yn_ * core
    dev2 = yn_ * (1 - core) + xn_ * core

    def load_shared(half):
        cols = pl.ds(half * inter, inter)
        return (pltpu.make_async_copy(sg.at[:, cols], wa.at[2 * half], sem_a.at[2 * half]),
                pltpu.make_async_copy(su.at[:, cols], wa.at[2 * half + 1], sem_a.at[2 * half + 1]))

    def load_expert(e):
        s = lax.rem(e, 2) * 2
        return (pltpu.make_async_copy(eg.at[e], wa.at[s], sem_a.at[s]),
                pltpu.make_async_copy(eu.at[e], wa.at[s + 1], sem_a.at[s + 1]))

    def load_down(c, j):
        cols = pl.ds(pl.multiple_of(c * CW, CW), CW)
        if j < n_loc:
            src = ed.at[j, :, cols]
        else:
            src = sd.at[pl.ds((j - n_loc) * inter, inter), cols]
        return pltpu.make_async_copy(src, wb.at[j], sem_b.at[j])

    def rcopy(src, dst, ssem, rsem, dev):
        return pltpu.make_async_remote_copy(src_ref=src, dst_ref=dst, send_sem=ssem, recv_sem=rsem,
                                            device_id={'ep': dev}, device_id_type=pl.DeviceIdType.MESH)

    for half in range(2):
        for cp in load_shared(half):
            cp.start()

    barrier = pltpu.get_barrier_semaphore()
    for k in range(1, n):
        pl.semaphore_signal(barrier, inc=1, device_id={'ep': lax.rem(me + k, n)}, device_id_type=pl.DeviceIdType.MESH)
    pl.semaphore_wait(barrier, n - 1)

    wt_cp = []
    for k in range(1, n):
        d = lax.rem(me + k, n)
        cp = rcopy(wt_ref.at[pl.ds(pl.multiple_of(d * n_loc, n_loc), n_loc)], wt_all.at[me],
                   wt_send.at[k], wt_recv.at[me], d)
        cp.start()
        wt_cp.append(cp)
    own = [rcopy(u_ref, u_all.at[me], g_send.at[i], g_recv.at[me], d) for i, d in enumerate((dev1, dev2, sib))]
    for cp in own:
        cp.start()
    u_all[me] = u_ref[...]
    wt_all[me] = wt_ref[pl.ds(pl.multiple_of(me * n_loc, n_loc), n_loc), :]

    def glu(lhs, gw, uw):
        g = jnp.dot(lhs, gw, preferred_element_type=F32)
        v = jnp.dot(lhs, uw, preferred_element_type=F32)
        return (g * (1.0 / (1.0 + jnp.exp(-g))) * v).astype(BF)

    cols_n = [(i, min(i + 256, inter)) for i in range(0, inter, 256)]

    for half in range(2):
        for cp in load_shared(half):
            cp.wait()
        for a, b in cols_n:
            act_sh[:, half * inter + a:half * inter + b] = glu(u_ref[...], wa[2 * half, :, a:b], wa[2 * half + 1, :, a:b])
        for cp in load_expert(half):
            cp.start()

    for k in range(1, n):
        s = lax.rem(me + k, n)
        rcopy(wt_all.at[s], wt_all.at[s], wt_send.at[0], wt_recv.at[s], sib).wait_recv()
    w_all = wt_all[...].reshape(n * n_loc, 128)
    ti = lax.broadcasted_iota(jnp.int32, (128, 128), 0)
    tj = lax.broadcasted_iota(jnp.int32, (128, 128), 1)
    tri = (ti < tj).astype(F32).astype(BF)
    hit = w_all > 0.0
    rank = jnp.dot(hit.astype(F32).astype(BF), tri, preferred_element_type=F32)
    rank_s[...] = jnp.where(hit, rank, -1000.0).reshape(n, n_loc, 128)
    row48 = lax.broadcasted_iota(jnp.int32, (2 * CAP, 256), 0).astype(F32)

    def tables(p, carry):
        for e in range(n_loc):
            rk = jnp.concatenate([rank_s[2 * p, e:e + 1, :], rank_s[2 * p + 1, e:e + 1, :] + float(CAP)], axis=1)
            ww = jnp.concatenate([wt_all[2 * p, e:e + 1, :], wt_all[2 * p + 1, e:e + 1, :]], axis=1)
            sel = row48 == rk
            pm[p, e * 2 * CAP:(e + 1) * 2 * CAP, :] = jnp.where(sel, 1.0, 0.0).astype(BF)
            wsel[e * 2 * CAP:(e + 1) * 2 * CAP, :] = jnp.where(sel, ww, 0.0)
        wt = wsel[...].T
        b1 = wt.astype(BF)
        r1 = wt - b1.astype(F32)
        b2 = r1.astype(BF)
        b3 = (r1 - b2.astype(F32)).astype(BF)
        cm[p, 0:256, :] = b1
        cm[p, 256:512, :] = b2
        cm[p, 512:768, :] = b3
        return carry

    lax.fori_loop(0, 4, tables, 0)

    def arrive(s):
        rcopy(u_all.at[s], u_all.at[s], g_send.at[0], g_recv.at[s], sib).wait_recv()

    def partner(s):
        return (s // 2) * 2 + 1 - lax.rem(s, 2)

    def dispatch(p):
        rows = pl.ds(pl.multiple_of(p * 2 * CAP, 16), 2 * CAP)
        for a in range(0, hid, 512):
            uv = u_all[pl.ds(2 * p, 2), :, a:a + 512].reshape(256, 512)
            r = jnp.dot(pm[p], uv, preferred_element_type=F32).astype(BF)
            for e in range(n_loc):
                xr[e, rows, a:a + 512] = r[e * 2 * CAP:(e + 1) * 2 * CAP]

    arrive(sib)
    dispatch(chip)
    arrive(dev1)
    rel = [rcopy(u_all.at[dev1], u_all.at[dev1], g_send.at[3], g_recv.at[dev1], dev2),
           rcopy(u_all.at[dev1], u_all.at[dev1], g_send.at[4], g_recv.at[dev1], sib)]
    rel[0].start()
    rel[1].start()
    arrive(dev2)
    rel.append(rcopy(u_all.at[dev2], u_all.at[dev2], g_send.at[5], g_recv.at[dev2], sib))
    rel[2].start()
    arrive(partner(dev1))
    dispatch(dev1 // 2)
    arrive(partner(dev2))
    dispatch(dev2 // 2)
    arrive(dg)
    rel.append(rcopy(u_all.at[dg], u_all.at[dg], g_send.at[6], g_recv.at[dg], sib))
    rel[3].start()
    arrive(partner(dg))
    dispatch(dg // 2)

    def gate_up(e, carry):
        s = lax.rem(e, 2) * 2
        for cp in load_expert(e):
            cp.wait()
        for a, b in cols_n:
            act[e, :, a:b] = glu(xr[e], wa[s, :, a:b], wa[s + 1, :, a:b])

        @pl.when(e + 2 < n_loc)
        def _():
            for cp in load_expert(e + 2):
                cp.start()

        @pl.when(e == n_loc - 3)
        def _():
            for j in range(n_loc + 2):
                load_down(0, j).start()
        return carry

    lax.fori_loop(0, n_loc, gate_up, 0)

    for cp in own + rel:
        cp.wait_send()
    for cp in wt_cp:
        cp.wait_send()

    def st1(c):
        return rcopy(part.at[lax.rem(c, 2), 1 - core], rx0.at[lax.rem(c, 4)], d_send.at[0, lax.rem(c, 2)], d_recv.at[0, lax.rem(c, 4)], sib)

    def st2(c):
        return rcopy(s1.at[lax.rem(c, 2)], rx1.at[lax.rem(c, 4)], d_send.at[1, lax.rem(c, 2)], d_recv.at[1, lax.rem(c, 4)], dev1)

    def st3(c):
        return rcopy(s2.at[lax.rem(c, 2)], rx2.at[c], d_send.at[2, lax.rem(c, 2)], d_recv.at[2, c], dev2)

    def st4(c):
        return rcopy(s3.at[lax.rem(c, 2)], rx3.at[c], d_send.at[3, lax.rem(c, 2)], d_recv.at[3, c], sib)

    def chunk(c, carry):
        @pl.when(c < nc)
        def _():
            sl = lax.rem(c, 2)
            cols = pl.ds(pl.multiple_of(c * CW, CW), CW)
            for e in range(n_loc):
                load_down(c, e).wait()
                o = jnp.dot(act[e], wb[e], preferred_element_type=F32).astype(BF)
                for p in range(4):
                    orow[p, e * 2 * CAP:(e + 1) * 2 * CAP, :] = o[p * 2 * CAP:(p + 1) * 2 * CAP]

                @pl.when(c + 1 < nc)
                def _():
                    load_down(c + 1, e).start()
            for j in (n_loc, n_loc + 1):
                load_down(c, j).wait()
            sh = (jnp.dot(act_sh[:, :inter], wb[n_loc], preferred_element_type=F32)
                  + jnp.dot(act_sh[:, inter:], wb[n_loc + 1], preferred_element_type=F32))
            ybase[:, cols] = h1_ref[:, cols].astype(F32) + sh

            @pl.when(c + 1 < nc)
            def _():
                for j in (n_loc, n_loc + 1):
                    load_down(c + 1, j).start()
            for dy in (1, 0):
                for dx in (1, 0):
                    py = (1 - cy) if dy else cy
                    px = (1 - cx) if dx else cx
                    p = py * 2 + px
                    r3 = jnp.dot(cm[p], orow[p], preferred_element_type=F32)
                    res = r3[0:256] + r3[256:512] + r3[512:768]
                    for h in range(2):
                        a, b = (dx, dy) if h == 0 else (dy, dx)
                        for cc in range(2):
                            part[sl, h, a, b, cc ^ h] = res[cc * 128:(cc + 1) * 128, h * 128:(h + 1) * 128]
            st1(c).start()

        @pl.when(jnp.logical_and(c >= 1, c < nc + 1))
        def _():
            k = c - 1
            sl = lax.rem(k, 2)
            st1(k).wait_recv()

            @pl.when(k >= 2)
            def _():
                st2(k - 2).wait_send()
            for b in range(2):
                for d in range(2):
                    s1[sl, b, d] = part[sl, core, 1, b, d] + rx0[lax.rem(k, 4), 1, b, d]
            st2(k).start()
            for b in range(2):
                for d in range(2):
                    keep0[sl, b, d] = part[sl, core, 0, b, d] + rx0[lax.rem(k, 4), 0, b, d]
            st1(k).wait_send()

        @pl.when(jnp.logical_and(c >= 2, c < nc + 2))
        def _():
            k = c - 2
            sl = lax.rem(k, 2)
            st2(k).wait_recv()

            @pl.when(k >= 2)
            def _():
                st3(k - 2).wait_send()
            for d in range(2):
                s2[sl, d] = keep0[sl, 1, d] + rx1[lax.rem(k, 4), 1, d]
            st3(k).start()
            for d in range(2):
                keep1[sl, d] = keep0[sl, 0, d] + rx1[lax.rem(k, 4), 0, d]

        @pl.when(jnp.logical_and(c >= 3, c < nc + 3))
        def _():
            k = c - 3
            sl = lax.rem(k, 2)
            st3(k).wait_recv()

            @pl.when(k >= 2)
            def _():
                st4(k - 2).wait_send()
            s3[sl] = keep1[sl, 1] + rx2[k, 1]
            st4(k).start()
            keep2[sl] = keep1[sl, 0] + rx2[k, 0]

        @pl.when(c >= 4)
        def _():
            k = c - 4
            sl = lax.rem(k, 2)
            mine = pl.ds(pl.multiple_of(k * CW + core * 128, 128), 128)
            other = pl.ds(pl.multiple_of(k * CW + (1 - core) * 128, 128), 128)
            st4(k).wait_recv()
            y_ref[:, mine] = (ybase[:, mine] + keep2[sl]).astype(BF)
            y_ref[:, other] = (ybase[:, other] + rx3[k]).astype(BF)
        return carry

    lax.fori_loop(0, nc + 4, chunk, 0)
    for k in (nc - 2, nc - 1):
        st2(k).wait_send()
        st3(k).wait_send()
        st4(k).wait_send()


def moe(u, h1, wt, s_gate, s_up, s_down, e_gate, e_up, e_down):
    t, hid = u.shape
    n_loc, _, inter = e_gate.shape
    nc = hid // CW
    V = pltpu.VMEM
    D = pltpu.SemaphoreType.DMA
    vm = pl.BlockSpec(memory_space=pltpu.VMEM)
    an = pl.BlockSpec(memory_space=pl.ANY)
    return pl.pallas_call(
        moe_kernel,
        out_shape=jax.ShapeDtypeStruct((t, hid), BF),
        in_specs=[vm] * 3 + [an] * 6,
        out_specs=vm,
        scratch_shapes=[
            V((8, t, hid), BF), V((8, n_loc, t), F32), V((8, n_loc, t), F32), V((n_loc * 2 * CAP, 256), F32),
            V((4, n_loc * 2 * CAP, 256), BF), V((4, 768, n_loc * 2 * CAP), BF),
            V((n_loc, 8 * CAP, hid), BF), V((n_loc, 8 * CAP, inter), BF), V((t, 2 * inter), BF),
            V((4, n_loc * 2 * CAP, CW), BF),
            V((4, hid, inter), BF), V((n_loc + 2, inter, CW), BF), V((t, hid), F32),
            V((2, 2, 2, 2, 2, t, 128), F32), V((4, 2, 2, 2, t, 128), F32), V((4, 2, 2, t, 128), F32),
            V((nc, 2, t, 128), F32), V((nc, t, 128), F32),
            V((2, 2, 2, t, 128), F32), V((2, 2, 2, t, 128), F32),
            V((2, 2, t, 128), F32), V((2, 2, t, 128), F32), V((2, t, 128), F32), V((2, t, 128), F32),
            D((4,)), D((n_loc + 2,)), D((8,)), D((8,)), D((7,)), D((8,)),
            D((4, 2)), D((4, nc)),
        ],
        compiler_params=pltpu.CompilerParams(collective_id=0, has_side_effects=True, vmem_limit_bytes=67043328),
        name='moe',
    )(u, h1, wt, s_gate, s_up, s_down, e_gate, e_up, e_down)


def solution(mesh):
    tok_spec = P(('rep', 'ep'))
    row_spec = P(('rep', 'ep'), None)
    cache_spec = P(('rep', 'ep'), None, None)
    exp_spec = P('ep', None, None)

    def local(x, cache, lens, ids, rw, w_q, w_dkv, w_uk, w_uv, w_o, s_gate, s_up, s_down, e_gate, e_up, e_down):
        n_exp = e_gate.shape[0] * mesh.shape['ep']
        wt = jnp.sum(jnp.where(ids.T[:, None, :] == jnp.arange(n_exp)[None, :, None], rw.T[:, None, :], 0.0), axis=0)
        h1, kv_new = attention(x, cache, lens, w_q, w_dkv, w_uk, w_uv, w_o)
        u = rms(h1).astype(jnp.bfloat16)
        y = moe(u, h1, wt, s_gate, s_up, s_down, e_gate, e_up, e_down)
        return y, kv_new

    in_specs = (row_spec, cache_spec, tok_spec, row_spec, row_spec) + (P(),) * 8 + (exp_spec,) * 3
    return jax.shard_map(local, mesh=mesh, in_specs=in_specs, out_specs=(row_spec, row_spec), check_vma=False)
```

```python
import jax
import jax.numpy as jnp
from jax import lax
from jax.experimental import pallas as pl
from jax.experimental.pallas import tpu as pltpu
from jax.sharding import PartitionSpec as P

EPS = 1e-6
ROPE_BASE = 1.0e4
BF = jnp.bfloat16
F32 = jnp.float32
CAP = 24
CW = 256
NA = 768
NSUB = 4


NB = 16
RING = 3


def attn_kernel(lens_ref, ids_ref, rw_ref, x_ref, cs_ref, sn_ref, wq_h, wdkv_h, wuk_h, wuv_h, wo_h, cache_h,
                h1_ref, u_ref, kvn_ref, wt_ref,
                wq, wdkv, wuk, wuv, wo, cbuf, qs, kvs, os, oc,
                sem_w, sem_q, sem_c):
    t, hid = x_ref.shape
    heads, nope, kvl = wuk.shape
    kvd = cbuf.shape[2]
    rot = kvd - kvl
    qkd = nope + rot
    length = cbuf.shape[3]
    vh = wuv.shape[2]
    nblk = t // NB
    qw = 4 * qkd
    nq = heads // 4
    scale = qkd ** -0.5

    cp_dkv = pltpu.make_async_copy(wdkv_h, wdkv, sem_w.at[0])
    cp_uk = pltpu.make_async_copy(wuk_h, wuk, sem_w.at[1])
    cp_uv = pltpu.make_async_copy(wuv_h, wuv, sem_w.at[2])
    cp_o = pltpu.make_async_copy(wo_h, wo, sem_w.at[3])
    cp_q = [pltpu.make_async_copy(wq_h.at[:, i * qw:(i + 1) * qw], wq.at[i], sem_q.at[i]) for i in range(nq)]

    def load(b):
        sl = lax.rem(b, RING)
        return pltpu.make_async_copy(cache_h.at[pl.ds(b * NB, NB)], cbuf.at[sl], sem_c.at[sl])

    cp_dkv.start()
    cp_q[0].start()
    cp_uk.start()
    for cp in cp_q[1:]:
        cp.start()
    for b in range(RING):
        load(b).start()
    cp_uv.start()
    cp_o.start()

    cs = cs_ref[...]
    sn = sn_ref[...]
    lane = lax.broadcasted_iota(jnp.int32, (t, 128), 1)
    low = lax.rem(lane, rot) < rot // 2

    def rope2(v):
        sw = jnp.where(low, pltpu.roll(v, 128 - rot // 2, 1), pltpu.roll(v, rot // 2, 1))
        return v * cs + sw * sn

    xf = x_ref[...].astype(F32)
    xn = (xf * lax.rsqrt(jnp.mean(xf * xf, axis=-1, keepdims=True) + EPS)).astype(BF)

    ex = lax.broadcasted_iota(jnp.int32, wt_ref.shape, 0)
    wt = jnp.zeros(wt_ref.shape, F32)
    for k in range(ids_ref.shape[0]):
        wt = wt + jnp.where(ids_ref[k:k + 1, :] == ex, rw_ref[k:k + 1, :], 0.0)
    wt_ref[...] = wt

    cp_dkv.wait()
    kv = lax.dot_general(xn, wdkv[...], (((1,), (1,)), ((), ())), preferred_element_type=F32)
    kl = kv[:, 0:kvl]
    kl = (kl * lax.rsqrt(jnp.mean(kl * kl, axis=-1, keepdims=True) + EPS)).astype(BF)
    kr = kv[:, kvl:kvd]
    kr = rope2(jnp.concatenate([kr, kr], axis=1)).astype(BF)
    kvs[:, 0:kvl] = kl.astype(F32)
    kvs[:, kvl:kvl + 128] = jnp.where(lane < rot, kr.astype(F32), 0.0)
    kvn_ref[...] = kvs[...].T[0:kvd].astype(BF)

    for i in range(nq):
        cp_q[i].wait()
        qc = jnp.dot(xn, wq[i], preferred_element_type=F32).astype(BF).astype(F32)
        if i == 0:
            cp_uk.wait()
        for j in range(2):
            o0 = j * 2 * qkd
            h = i * 4 + j * 2
            n0 = qc[:, o0:o0 + nope].astype(BF)
            n1 = qc[:, o0 + qkd:o0 + qkd + nope].astype(BF)
            r = jnp.concatenate([qc[:, o0 + nope:o0 + qkd], qc[:, o0 + qkd + nope:o0 + 2 * qkd]], axis=1)
            r = rope2(r).astype(BF).astype(F32)
            qs[:, h, 0:kvl] = jnp.dot(n0, wuk[h], preferred_element_type=F32).astype(BF).astype(F32)
            qs[:, h + 1, 0:kvl] = jnp.dot(n1, wuk[h + 1], preferred_element_type=F32).astype(BF).astype(F32)
            qs[:, h, kvl:kvl + 128] = jnp.where(lane < rot, r, 0.0)
            qs[:, h + 1, kvl:kvl + 128] = jnp.where(lane < rot, pltpu.roll(r, rot, 1), 0.0)

    pos = lax.broadcasted_iota(jnp.int32, (heads, length), 1)

    def block(b, carry):
        sl = lax.rem(b, RING)
        load(b).wait()
        ss = []
        sns = []
        for i in range(NB):
            qf = qs[b * NB + i]
            qb = qf[:, 0:kvd].astype(BF)
            ss.append(jnp.dot(qb, cbuf[sl, i], preferred_element_type=F32))
            sns.append(jnp.sum(qf * kvs[pl.ds(b * NB + i, 1), :], axis=1, keepdims=True) * scale)
        for i in range(NB):
            s = jnp.where(pos < lens_ref[b * NB + i], ss[i] * scale, -jnp.inf)
            mx = jnp.maximum(jnp.max(s, axis=1, keepdims=True), sns[i])
            e = jnp.exp(s - mx)
            en = jnp.exp(sns[i] - mx)
            den = jnp.sum(e, axis=1, keepdims=True) + en
            p = (e / den).astype(BF)
            pn = (en / den).astype(BF).astype(F32)
            o = lax.dot_general(p, cbuf[sl, i, 0:kvl, :], (((1,), (1,)), ((), ())), preferred_element_type=F32)
            os[:, b * NB + i, :] = o + pn * kvs[pl.ds(b * NB + i, 1), 0:kvl]

        @pl.when(b + RING < nblk)
        def _():
            load(b + RING).start()
        return carry

    lax.fori_loop(0, nblk, block, 0)

    cp_uv.wait()
    for h in range(heads):
        oc[:, h * vh:(h + 1) * vh] = jnp.dot(os[h].astype(BF), wuv[h], preferred_element_type=F32).astype(BF)
    cp_o.wait()
    ssq = jnp.zeros((t, 1), F32)
    for a in range(0, hid, 512):
        h1 = (x_ref[:, a:a + 512].astype(F32)
              + jnp.dot(oc[...], wo[:, a:a + 512], preferred_element_type=F32)).astype(BF)
        h1_ref[:, a:a + 512] = h1
        hf = h1.astype(F32)
        ssq = ssq + jnp.sum(hf * hf, axis=1, keepdims=True)
    inv = lax.rsqrt(ssq * (1.0 / hid) + EPS)
    u_ref[...] = (h1_ref[...].astype(F32) * inv).astype(BF)


def attention(x, cache, lens, ids, rw, n_exp, w_q, w_dkv, w_uk, w_uv, w_o):
    t, hid = x.shape
    heads, nope, kvl = w_uk.shape
    _, length, kvd = cache.shape
    vh = w_uv.shape[2]
    rot = kvd - kvl
    half = rot // 2
    lane = jnp.arange(128)
    ang = lens.astype(F32)[:, None] * (ROPE_BASE ** (-2.0 * (lane % half).astype(F32) / rot))[None, :]
    cs4 = jnp.cos(ang)
    sn4 = jnp.sin(ang) * jnp.where(lane % rot < half, -1.0, 1.0)[None, :]
    V = pltpu.VMEM
    D = pltpu.SemaphoreType.DMA
    vm = pl.BlockSpec(memory_space=pltpu.VMEM)
    an = pl.BlockSpec(memory_space=pl.ANY)
    h1, u, kvt, wt = pl.pallas_call(
        attn_kernel,
        out_shape=(jax.ShapeDtypeStruct((t, hid), BF), jax.ShapeDtypeStruct((t, hid), BF),
                   jax.ShapeDtypeStruct((kvd, t), BF), jax.ShapeDtypeStruct((n_exp, t), F32)),
        in_specs=[pl.BlockSpec(memory_space=pltpu.SMEM)] + [vm] * 5 + [an] * 6,
        out_specs=(vm, vm, vm, vm),
        scratch_shapes=[
            V((heads // 4, hid, 4 * (nope + rot)), BF), V((kvd, hid), BF), V((heads, nope, kvl), BF),
            V((heads, kvl, vh), BF), V((heads * vh, hid), BF), V((RING, NB, kvd, length), BF),
            V((t, heads, kvl + 128), F32), V((t, kvl + 128), F32), V((heads, t, kvl), F32), V((t, heads * vh), BF),
            D((4,)), D((heads // 4,)), D((RING,)),
        ],
        compiler_params=pltpu.CompilerParams(vmem_limit_bytes=67043328),
        name='attn',
    )(lens, ids.T, rw.T, x, cs4, sn4, w_q, w_dkv.T, w_uk, w_uv, w_o, cache.transpose(0, 2, 1))
    return h1, u, kvt.T, wt


def moe_kernel(u_ref, h1_ref, wt_ref, sg, su, sd, eg, eu, ed, y_ref,
               u_all, wt_all, rank_s, wsel, pm, cm, xr, act, act_sh, orow, wa, wc, wb, ybase,
               part, rx0, rx1, rx2, rx3, s1, keep0, s2, keep1, s3, keep2,
               sem_a, sem_b, wt_send, wt_recv, g_send, g_recv,
               d_send, d_recv):
    n = 8
    n_loc = 8
    hid = u_ref.shape[1]
    inter = act.shape[2]
    na = wa.shape[3]
    nc = hid // CW
    me = lax.axis_index('ep')
    core = lax.rem(me, 2)
    chip = me // 2
    cx = lax.rem(chip, 2)
    cy = chip // 2
    sib = chip * 2 + 1 - core
    xn_ = (cy * 2 + 1 - cx) * 2 + core
    yn_ = ((1 - cy) * 2 + cx) * 2 + core
    dg = ((1 - cy) * 2 + 1 - cx) * 2 + core
    dev1 = xn_ * (1 - core) + yn_ * core
    dev2 = yn_ * (1 - core) + xn_ * core

    def load_unit(srcs, base, slot, part_):
        buf, width, off = (wa, na, 0) if part_ == 0 else (wc, inter - na, na)
        return [pltpu.make_async_copy(src.at[:, pl.ds(base + off, width)], buf.at[slot, i], sem_a.at[part_, slot, i])
                for i, src in enumerate(srcs)]

    def load_shared(half, part_):
        return load_unit((sg, su), half * inter, half, part_)

    def load_expert(e, part_):
        return load_unit((eg.at[e], eu.at[e]), 0, lax.rem(e, 2), part_)

    def load_down(c, j):
        cols = pl.ds(pl.multiple_of(c * CW, CW), CW)
        if j < n_loc:
            src = ed.at[j, :, cols]
        else:
            src = sd.at[pl.ds((j - n_loc) * inter, inter), cols]
        return pltpu.make_async_copy(src, wb.at[j], sem_b.at[j])

    def rcopy(src, dst, ssem, rsem, dev):
        return pltpu.make_async_remote_copy(src_ref=src, dst_ref=dst, send_sem=ssem, recv_sem=rsem,
                                            device_id={'ep': dev}, device_id_type=pl.DeviceIdType.MESH)

    for half in range(2):
        for part_ in range(2):
            for cp in load_shared(half, part_):
                cp.start()

    barrier = pltpu.get_barrier_semaphore()
    for k in range(1, n):
        pl.semaphore_signal(barrier, inc=1, device_id={'ep': lax.rem(me + k, n)}, device_id_type=pl.DeviceIdType.MESH)
    pl.semaphore_wait(barrier, n - 1)

    wt_cp = []
    for k in range(1, n):
        d = lax.rem(me + k, n)
        cp = rcopy(wt_ref.at[pl.ds(pl.multiple_of(d * n_loc, n_loc), n_loc)], wt_all.at[me],
                   wt_send.at[k], wt_recv.at[me], d)
        cp.start()
        wt_cp.append(cp)
    rsub = u_ref.shape[0] // NSUB

    def ucopy(kind, s, i, dev, src=None):
        rows = pl.ds(i * rsub, rsub)
        return rcopy(u_all.at[s, rows] if src is None else src.at[rows], u_all.at[s, rows],
                     g_send.at[kind, i], g_recv.at[s, i], dev)

    own = [ucopy(kind, me, i, d, u_ref) for i in range(NSUB) for kind, d in enumerate((dev1, dev2, sib))]
    for cp in own:
        cp.start()
    u_all[me] = u_ref[...]
    wt_all[me] = wt_ref[pl.ds(pl.multiple_of(me * n_loc, n_loc), n_loc), :]

    def glu(lhs, gw, uw):
        g = jnp.dot(lhs, gw, preferred_element_type=F32)
        v = jnp.dot(lhs, uw, preferred_element_type=F32)
        return (g * (1.0 / (1.0 + jnp.exp(-g))) * v).astype(BF)

    def glu_unit(lhs, slot, part_, store):
        buf, width, off = (wa, na, 0) if part_ == 0 else (wc, inter - na, na)
        for a in range(0, width, 256):
            b = min(a + 256, width)
            store(off + a, off + b, glu(lhs, buf[slot, 0, :, a:b], buf[slot, 1, :, a:b]))

    for half in range(2):
        for part_ in range(2):
            for cp in load_shared(half, part_):
                cp.wait()

            def put(a, b, v):
                act_sh[:, half * inter + a:half * inter + b] = v

            glu_unit(u_ref[...], half, part_, put)
            for cp in load_expert(half, part_):
                cp.start()

    for k in range(1, n):
        s = lax.rem(me + k, n)
        rcopy(wt_all.at[s], wt_all.at[s], wt_send.at[0], wt_recv.at[s], sib).wait_recv()
    w_all = wt_all[...].reshape(n * n_loc, 128)
    ti = lax.broadcasted_iota(jnp.int32, (128, 128), 0)
    tj = lax.broadcasted_iota(jnp.int32, (128, 128), 1)
    tri = (ti < tj).astype(F32).astype(BF)
    hit = w_all > 0.0
    rank = jnp.dot(hit.astype(F32).astype(BF), tri, preferred_element_type=F32)
    rank_s[...] = jnp.where(hit, rank, -1000.0).reshape(n, n_loc, 128)
    row48 = lax.broadcasted_iota(jnp.int32, (2 * CAP, 256), 0).astype(F32)

    def tables(p, carry):
        for e in range(n_loc):
            rk = jnp.concatenate([rank_s[2 * p, e:e + 1, :], rank_s[2 * p + 1, e:e + 1, :] + float(CAP)], axis=1)
            ww = jnp.concatenate([wt_all[2 * p, e:e + 1, :], wt_all[2 * p + 1, e:e + 1, :]], axis=1)
            sel = row48 == rk
            pm[p, e * 2 * CAP:(e + 1) * 2 * CAP, :] = jnp.where(sel, 1.0, 0.0).astype(BF)
            wsel[e * 2 * CAP:(e + 1) * 2 * CAP, :] = jnp.where(sel, ww, 0.0)
        wt = wsel[...].T
        b1 = wt.astype(BF)
        r1 = wt - b1.astype(F32)
        b2 = r1.astype(BF)
        b3 = (r1 - b2.astype(F32)).astype(BF)
        cm[p, 0:256, :] = b1
        cm[p, 256:512, :] = b2
        cm[p, 512:768, :] = b3
        return carry

    lax.fori_loop(0, 4, tables, 0)

    def arrive(s, subs=range(NSUB)):
        for i in subs:
            ucopy(0, s, i, sib).wait_recv()

    def partner(s):
        return (s // 2) * 2 + 1 - lax.rem(s, 2)

    def dispatch(p):
        rows = pl.ds(pl.multiple_of(p * 2 * CAP, 16), 2 * CAP)
        for a in range(0, hid, 512):
            uv = u_all[pl.ds(2 * p, 2), :, a:a + 512].reshape(256, 512)
            r = jnp.dot(pm[p], uv, preferred_element_type=F32).astype(BF)
            for e in range(n_loc):
                xr[e, rows, a:a + 512] = r[e * 2 * CAP:(e + 1) * 2 * CAP]

    rel = []

    def relay(kinds, s, devs, i):
        arrive(s, (i,))
        for kind, dev in zip(kinds, devs):
            cp = ucopy(kind, s, i, dev)
            cp.start()
            rel.append(cp)

    arrive(sib)
    dispatch(chip)
    for i in range(NSUB):
        relay((3, 4), dev1, (dev2, sib), i)
        relay((5,), dev2, (sib,), i)
    arrive(partner(dev1))
    dispatch(dev1 // 2)
    arrive(partner(dev2))
    dispatch(dev2 // 2)
    for i in range(NSUB):
        relay((6,), dg, (sib,), i)
    arrive(partner(dg))
    dispatch(dg // 2)

    def gate_up(e, carry):
        def put(a, b, v):
            act[e, :, a:b] = v

        for part_ in range(2):
            for cp in load_expert(e, part_):
                cp.wait()
            glu_unit(xr[e], lax.rem(e, 2), part_, put)

            @pl.when(e + 2 < n_loc)
            def _():
                for cp in load_expert(e + 2, part_):
                    cp.start()

        @pl.when(e == n_loc - 3)
        def _():
            for j in range(n_loc + 2):
                load_down(0, j).start()
        return carry

    lax.fori_loop(0, n_loc, gate_up, 0)

    for cp in own + rel:
        cp.wait_send()
    for cp in wt_cp:
        cp.wait_send()

    def st1(c):
        return rcopy(part.at[lax.rem(c, 2), 1 - core], rx0.at[lax.rem(c, 4)], d_send.at[0, lax.rem(c, 2)], d_recv.at[0, lax.rem(c, 4)], sib)

    def st2(c):
        return rcopy(s1.at[lax.rem(c, 2)], rx1.at[lax.rem(c, 4)], d_send.at[1, lax.rem(c, 2)], d_recv.at[1, lax.rem(c, 4)], dev1)

    def st3(c):
        return rcopy(s2.at[lax.rem(c, 2)], rx2.at[c], d_send.at[2, lax.rem(c, 2)], d_recv.at[2, c], dev2)

    def st4(c):
        return rcopy(s3.at[lax.rem(c, 2)], rx3.at[c], d_send.at[3, lax.rem(c, 2)], d_recv.at[3, c], sib)

    def refill(c, grp):
        @pl.when(c + 1 < nc)
        def _():
            for j in grp:
                load_down(c + 1, j).start()

    def down(c, grp):
        for j in grp:
            load_down(c, j).wait()
        outs = [jnp.dot(act[e], wb[e], preferred_element_type=F32).astype(BF) for e in grp]
        for e, o in zip(grp, outs):
            for p in range(4):
                orow[p, e * 2 * CAP:(e + 1) * 2 * CAP, :] = o[p * 2 * CAP:(p + 1) * 2 * CAP]
        refill(c, grp)

    def combine(c):
        sl = lax.rem(c, 2)
        for dy in (1, 0):
            for dx in (1, 0):
                py = (1 - cy) if dy else cy
                px = (1 - cx) if dx else cx
                p = py * 2 + px
                r3 = jnp.dot(cm[p], orow[p], preferred_element_type=F32)
                res = r3[0:256] + r3[256:512] + r3[512:768]
                for h in range(2):
                    a, b = (dx, dy) if h == 0 else (dy, dx)
                    for cc in range(2):
                        part[sl, h, a, b, cc ^ h] = res[cc * 128:(cc + 1) * 128, h * 128:(h + 1) * 128]
        st1(c).start()

    def shared_down(c):
        cols = pl.ds(pl.multiple_of(c * CW, CW), CW)
        grp = (n_loc, n_loc + 1)
        for j in grp:
            load_down(c, j).wait()
        sh = (jnp.dot(act_sh[:, :inter], wb[n_loc], preferred_element_type=F32)
              + jnp.dot(act_sh[:, inter:], wb[n_loc + 1], preferred_element_type=F32))
        ybase[:, cols] = h1_ref[:, cols].astype(F32) + sh
        refill(c, grp)

    def stage2(k):
        sl = lax.rem(k, 2)
        st1(k).wait_recv()

        @pl.when(k >= 2)
        def _():
            st2(k - 2).wait_send()
        for b in range(2):
            for d in range(2):
                s1[sl, b, d] = part[sl, core, 1, b, d] + rx0[lax.rem(k, 4), 1, b, d]
        st2(k).start()
        for b in range(2):
            for d in range(2):
                keep0[sl, b, d] = part[sl, core, 0, b, d] + rx0[lax.rem(k, 4), 0, b, d]
        st1(k).wait_send()

    def stage3(k):
        sl = lax.rem(k, 2)
        st2(k).wait_recv()

        @pl.when(k >= 2)
        def _():
            st3(k - 2).wait_send()
        for d in range(2):
            s2[sl, d] = keep0[sl, 1, d] + rx1[lax.rem(k, 4), 1, d]
        st3(k).start()
        for d in range(2):
            keep1[sl, d] = keep0[sl, 0, d] + rx1[lax.rem(k, 4), 0, d]

    def stage4(k):
        sl = lax.rem(k, 2)
        st3(k).wait_recv()

        @pl.when(k >= 2)
        def _():
            st4(k - 2).wait_send()
        s3[sl] = keep1[sl, 1] + rx2[k, 1]
        st4(k).start()
        keep2[sl] = keep1[sl, 0] + rx2[k, 0]

    def stage5(k):
        mine = pl.ds(pl.multiple_of(k * CW + core * 128, 128), 128)
        other = pl.ds(pl.multiple_of(k * CW + (1 - core) * 128, 128), 128)
        st4(k).wait_recv()
        y_ref[:, mine] = (ybase[:, mine] + keep2[lax.rem(k, 2)]).astype(BF)
        y_ref[:, other] = (ybase[:, other] + rx3[k]).astype(BF)

    def chunk(c, carry):
        live = c < nc
        pl.when(live)(lambda: down(c, (0, 1, 2, 3)))
        pl.when(jnp.logical_and(c >= 1, c < nc + 1))(lambda: stage2(c - 1))
        pl.when(live)(lambda: down(c, (4, 5, 6, 7)))
        pl.when(jnp.logical_and(c >= 2, c < nc + 2))(lambda: stage3(c - 2))
        pl.when(live)(lambda: combine(c))
        pl.when(live)(lambda: shared_down(c))
        pl.when(jnp.logical_and(c >= 3, c < nc + 3))(lambda: stage4(c - 3))
        pl.when(c >= 4)(lambda: stage5(c - 4))
        return carry

    lax.fori_loop(0, nc + 4, chunk, 0)
    for k in (nc - 2, nc - 1):
        st2(k).wait_send()
        st3(k).wait_send()
        st4(k).wait_send()


def moe(u, h1, wt, s_gate, s_up, s_down, e_gate, e_up, e_down):
    t, hid = u.shape
    n_loc, _, inter = e_gate.shape
    nc = hid // CW
    V = pltpu.VMEM
    D = pltpu.SemaphoreType.DMA
    vm = pl.BlockSpec(memory_space=pltpu.VMEM)
    an = pl.BlockSpec(memory_space=pl.ANY)
    return pl.pallas_call(
        moe_kernel,
        out_shape=jax.ShapeDtypeStruct((t, hid), BF),
        in_specs=[vm] * 3 + [an] * 6,
        out_specs=vm,
        scratch_shapes=[
            V((8, t, hid), BF), V((8, n_loc, t), F32), V((8, n_loc, t), F32), V((n_loc * 2 * CAP, 256), F32),
            V((4, n_loc * 2 * CAP, 256), BF), V((4, 768, n_loc * 2 * CAP), BF),
            V((n_loc, 8 * CAP, hid), BF), V((n_loc, 8 * CAP, inter), BF), V((t, 2 * inter), BF),
            V((4, n_loc * 2 * CAP, CW), BF),
            V((2, 2, hid, NA), BF), V((2, 2, hid, inter - NA), BF), V((n_loc + 2, inter, CW), BF), V((t, hid), F32),
            V((2, 2, 2, 2, 2, t, 128), F32), V((4, 2, 2, 2, t, 128), F32), V((4, 2, 2, t, 128), F32),
            V((nc, 2, t, 128), F32), V((nc, t, 128), F32),
            V((2, 2, 2, t, 128), F32), V((2, 2, 2, t, 128), F32),
            V((2, 2, t, 128), F32), V((2, 2, t, 128), F32), V((2, t, 128), F32), V((2, t, 128), F32),
            D((2, 2, 2)), D((n_loc + 2,)), D((8,)), D((8,)), D((7, NSUB)), D((8, NSUB)),
            D((4, 2)), D((4, nc)),
        ],
        compiler_params=pltpu.CompilerParams(collective_id=0, has_side_effects=True, vmem_limit_bytes=67043328),
        name='moe',
    )(u, h1, wt, s_gate, s_up, s_down, e_gate, e_up, e_down)


def solution(mesh):
    tok_spec = P(('rep', 'ep'))
    row_spec = P(('rep', 'ep'), None)
    cache_spec = P(('rep', 'ep'), None, None)
    exp_spec = P('ep', None, None)

    def local(x, cache, lens, ids, rw, w_q, w_dkv, w_uk, w_uv, w_o, s_gate, s_up, s_down, e_gate, e_up, e_down):
        n_exp = e_gate.shape[0] * mesh.shape['ep']
        h1, u, kv_new, wt = attention(x, cache, lens, ids, rw, n_exp, w_q, w_dkv, w_uk, w_uv, w_o)
        y = moe(u, h1, wt, s_gate, s_up, s_down, e_gate, e_up, e_down)
        return y, kv_new

    in_specs = (row_spec, cache_spec, tok_spec, row_spec, row_spec) + (P(),) * 8 + (exp_spec,) * 3
    return jax.shard_map(local, mesh=mesh, in_specs=in_specs, out_specs=(row_spec, row_spec), check_vma=False)
```

```python
import jax
import jax.numpy as jnp
from jax import lax
from jax.experimental import pallas as pl
from jax.experimental.pallas import tpu as pltpu
from jax.sharding import PartitionSpec as P

EPS = 1e-6
ROPE_BASE = 1.0e4
BF = jnp.bfloat16
F32 = jnp.float32
CAP = 24
CW = 256
NA = 768
NSUB = 4


NB = 16
RING = 2
CW = 256
NA = 768
NSUB = 4


def layer_kernel(lens_ref, ids_ref, rw_ref, x_ref, cs_ref, sn_ref, wq_h, wdkv_h, wuk_h, wuv_h, wo_h, cache_h,
                 sg, su, sd, eg, eu, ed,
                 y_ref, kvn_ref,
                 u_all, wt_ref, wt_all, h1_ref, wa, wc0, rx0, rx1, rx2, rx3,
                 sem_w, sem_q, sem_c, sem_a, sem_b, wt_send, wt_recv, g_send, g_recv, d_send, d_recv):
    n = 8
    n_loc = eg.shape[0]
    t, hid = x_ref.shape
    inter = eg.shape[2]
    nc = hid // CW
    na = NA
    rsub = t // NSUB
    me = lax.axis_index('ep')
    core = lax.rem(me, 2)
    chip = me // 2
    cx = lax.rem(chip, 2)
    cy = chip // 2
    sib = chip * 2 + 1 - core
    xn_ = (cy * 2 + 1 - cx) * 2 + core
    yn_ = ((1 - cy) * 2 + cx) * 2 + core
    dg = ((1 - cy) * 2 + 1 - cx) * 2 + core
    dev1 = xn_ * (1 - core) + yn_ * core
    dev2 = yn_ * (1 - core) + xn_ * core

    def rcopy(src, dst, ssem, rsem, dev):
        return pltpu.make_async_remote_copy(src_ref=src, dst_ref=dst, send_sem=ssem, recv_sem=rsem,
                                            device_id={'ep': dev}, device_id_type=pl.DeviceIdType.MESH)

    def ucopy(kind, s, i, dev):
        rows = pl.ds(i * rsub, rsub)
        return rcopy(u_all.at[s, rows], u_all.at[s, rows], g_send.at[kind, i], g_recv.at[s, i], dev)

    def arrive(s, subs=range(NSUB)):
        for i in subs:
            ucopy(0, s, i, sib).wait_recv()

    def partner(s):
        return (s // 2) * 2 + 1 - lax.rem(s, 2)

    def wt_copy(k):
        d = lax.rem(me + k, n)
        return rcopy(wt_ref.at[pl.ds(pl.multiple_of(d * n_loc, n_loc), n_loc)], wt_all.at[me],
                     wt_send.at[k], wt_recv.at[me], d)

    def relay(kinds, s, devs, subs):
        for i in subs:
            arrive(s, (i,))
            for kind, dev in zip(kinds, devs):
                cp = ucopy(kind, s, i, dev)
                cp.start()

    def load_unit(srcs, base, slot, part_, wc1):
        if part_ == 0:
            dst, width, off = [wa.at[2 * slot], wa.at[2 * slot + 1]], na, 0
        else:
            buf = wc1 if slot else wc0
            dst, width, off = [buf.at[0], buf.at[1]], inter - na, na
        return [pltpu.make_async_copy(src.at[:, pl.ds(base + off, width)], d, sem_a.at[part_, slot, i])
                for i, (src, d) in enumerate(zip(srcs, dst))]

    def load_shared(half, part_, wc1=None):
        return load_unit((sg, su), half * inter, half, part_, wc1)

    def relay_near(i):
        relay((3, 4), dev1, (dev2, sib), (i,))
        relay((5,), dev2, (sib,), (i,))

    na_blk = t * 3 // 4 // NB

    def attn_scope(wdkv, wuk, wuv, wo, cbuf, qs, kvs, os, oc):
        heads, nope, kvl = wuk.shape
        kvd = cbuf.shape[2]
        rot = kvd - kvl
        qkd = nope + rot
        length = cbuf.shape[3]
        vh = wuv.shape[2]
        nblk = t // NB
        qw = 4 * qkd
        nq = heads // 4
        scale = qkd ** -0.5

        cp_dkv = pltpu.make_async_copy(wdkv_h, wdkv, sem_w.at[0])
        cp_uk = pltpu.make_async_copy(wuk_h, wuk, sem_w.at[1])
        cp_uv = pltpu.make_async_copy(wuv_h, wuv, sem_w.at[2])
        cp_o = pltpu.make_async_copy(wo_h, wo, sem_w.at[3])
        cp_q = [pltpu.make_async_copy(wq_h.at[:, i * qw:(i + 1) * qw], wa.at[i], sem_q.at[i]) for i in range(nq)]

        def load(b):
            sl = lax.rem(b, RING)
            return pltpu.make_async_copy(cache_h.at[pl.ds(b * NB, NB)], cbuf.at[sl], sem_c.at[sl])

        cp_dkv.start()
        cp_q[0].start()
        cp_uk.start()
        for cp in cp_q[1:]:
            cp.start()
        for b in range(RING):
            load(b).start()
        cp_uv.start()
        cp_o.start()

        barrier = pltpu.get_barrier_semaphore()
        for k in range(1, n):
            pl.semaphore_signal(barrier, inc=1, device_id={'ep': lax.rem(me + k, n)}, device_id_type=pl.DeviceIdType.MESH)
        pl.semaphore_wait(barrier, n - 1)

        ex = lax.broadcasted_iota(jnp.int32, wt_ref.shape, 0)
        wt = jnp.zeros(wt_ref.shape, F32)
        for k in range(ids_ref.shape[0]):
            wt = wt + jnp.where(ids_ref[k:k + 1, :] == ex, rw_ref[k:k + 1, :], 0.0)
        wt_ref[...] = wt
        wt_all[me] = wt_ref[pl.ds(pl.multiple_of(me * n_loc, n_loc), n_loc), :]
        cs = cs_ref[...]
        sn = sn_ref[...]
        lane = lax.broadcasted_iota(jnp.int32, (t, 128), 1)
        low = lax.rem(lane, rot) < rot // 2

        def rope2(v):
            sw = jnp.where(low, pltpu.roll(v, 128 - rot // 2, 1), pltpu.roll(v, rot // 2, 1))
            return v * cs + sw * sn

        xf = x_ref[...].astype(F32)
        xn = (xf * lax.rsqrt(jnp.mean(xf * xf, axis=-1, keepdims=True) + EPS)).astype(BF)

        cp_dkv.wait()
        kv = lax.dot_general(xn, wdkv[...], (((1,), (1,)), ((), ())), preferred_element_type=F32)
        kl = kv[:, 0:kvl]
        kl = (kl * lax.rsqrt(jnp.mean(kl * kl, axis=-1, keepdims=True) + EPS)).astype(BF)
        kr = kv[:, kvl:kvd]
        kr = rope2(jnp.concatenate([kr, kr], axis=1)).astype(BF)
        kvs[:, 0:kvl] = kl.astype(F32)
        kvs[:, kvl:kvl + 128] = jnp.where(lane < rot, kr.astype(F32), 0.0)
        kvn_ref[...] = kvs[...].T[0:kvd].astype(BF)

        for k in range(1, n):
            wt_copy(k).start()

        for i in range(nq):
            cp_q[i].wait()
            qc = jnp.dot(xn, wa[i], preferred_element_type=F32).astype(BF).astype(F32)
            if i == 0:
                cp_uk.wait()
            for j in range(2):
                o0 = j * 2 * qkd
                h = i * 4 + j * 2
                n0 = qc[:, o0:o0 + nope].astype(BF)
                n1 = qc[:, o0 + qkd:o0 + qkd + nope].astype(BF)
                r = jnp.concatenate([qc[:, o0 + nope:o0 + qkd], qc[:, o0 + qkd + nope:o0 + 2 * qkd]], axis=1)
                r = rope2(r).astype(BF).astype(F32)
                qs[:, h, 0:kvl] = jnp.dot(n0, wuk[h], preferred_element_type=F32).astype(BF).astype(F32)
                qs[:, h + 1, 0:kvl] = jnp.dot(n1, wuk[h + 1], preferred_element_type=F32).astype(BF).astype(F32)
                qs[:, h, kvl:kvl + 128] = jnp.where(lane < rot, r, 0.0)
                qs[:, h + 1, kvl:kvl + 128] = jnp.where(lane < rot, pltpu.roll(r, rot, 1), 0.0)

        pos = lax.broadcasted_iota(jnp.int32, (heads, length), 1)

        def block(b, carry):
            sl = lax.rem(b, RING)
            load(b).wait()
            ss = []
            sns = []
            for i in range(NB):
                qf = qs[b * NB + i]
                qb = qf[:, 0:kvd].astype(BF)
                ss.append(jnp.dot(qb, cbuf[sl, i], preferred_element_type=F32))
                sns.append(jnp.sum(qf * kvs[pl.ds(b * NB + i, 1), :], axis=1, keepdims=True) * scale)
            for i in range(NB):
                s = jnp.where(pos < lens_ref[b * NB + i], ss[i] * scale, -jnp.inf)
                mx = jnp.maximum(jnp.max(s, axis=1, keepdims=True), sns[i])
                e = jnp.exp(s - mx)
                en = jnp.exp(sns[i] - mx)
                den = jnp.sum(e, axis=1, keepdims=True) + en
                p = (e / den).astype(BF)
                pn = (en / den).astype(BF).astype(F32)
                o = lax.dot_general(p, cbuf[sl, i, 0:kvl, :], (((1,), (1,)), ((), ())), preferred_element_type=F32)
                os[:, lax.rem(b, na_blk) * NB + i, :] = o + pn * kvs[pl.ds(b * NB + i, 1), 0:kvl]

            @pl.when(b + RING < nblk)
            def _():
                load(b + RING).start()

            for j, cp in enumerate(load_shared(0, 0) + load_shared(1, 0) + load_shared(0, 1)):
                pl.when(b == j + 2)(cp.start)
            return carry

        for half in range(2):
            lax.fori_loop((0, na_blk)[half], (na_blk, nblk)[half], block, 0)
            if half == 0:
                cp_uv.wait()
                cp_o.wait()
            else:
                relay_near(0)
            rows = slice((0, na_blk * NB)[half], (na_blk * NB, t)[half])
            nh = rows.stop - rows.start
            for h in range(heads):
                oc[0:nh, h * vh:(h + 1) * vh] = jnp.dot(os[h, 0:nh].astype(BF), wuv[h], preferred_element_type=F32).astype(BF)
            ssq = jnp.zeros((nh, 1), F32)
            for a in range(0, hid, 512):
                h1 = (x_ref[rows, a:a + 512].astype(F32)
                      + jnp.dot(oc[0:nh], wo[:, a:a + 512], preferred_element_type=F32)).astype(BF)
                h1_ref[rows, a:a + 512] = h1
                hf = h1.astype(F32)
                ssq = ssq + jnp.sum(hf * hf, axis=1, keepdims=True)
            inv = lax.rsqrt(ssq * (1.0 / hid) + EPS)
            u_all[me, rows, :] = (h1_ref[rows, :].astype(F32) * inv).astype(BF)
            for i in range(rows.start // rsub, rows.stop // rsub):
                for kind, d in enumerate((dev1, dev2, sib)):
                    cp = ucopy(kind, me, i, d)
                    cp.start()

    heads, nope, kvl = wuk_h.shape
    vh = wuv_h.shape[2]
    _, kvd, length = cache_h.shape
    V = pltpu.VMEM
    pl.run_scoped(
        attn_scope,
        V((kvd, hid), BF), V((heads, nope, kvl), BF),
        V((heads, kvl, vh), BF), V((heads * vh, hid), BF), V((RING, NB, kvd, length), BF),
        V((t, heads, kvl + 128), F32), V((t, kvl + 128), F32), V((heads, na_blk * NB, kvl), F32), V((na_blk * NB, heads * vh), BF))

    def moe_scope(rank_s, wsel, pm, cm, xr, act, act_sh, orow, wc1, wb, ybase,
                  part, s1, keep0, s2, keep1, s3, keep2):
        def load_expert(e, slot, part_):
            return load_unit((eg.at[e], eu.at[e]), 0, slot, part_, wc1)

        def load_routed(c, e):
            cols = pl.ds(pl.multiple_of(c * CW, CW), CW)
            return pltpu.make_async_copy(ed.at[e, :, cols], wb.at[e], sem_b.at[e])

        def load_down(c, j):
            cols = pl.ds(pl.multiple_of(c * CW, CW), CW)
            if j < n_loc:
                src = ed.at[j, :, cols]
            else:
                src = sd.at[pl.ds((j - n_loc) * inter, inter), cols]
            return pltpu.make_async_copy(src, wb.at[j], sem_b.at[j])

        for cp in load_shared(1, 1, wc1):
            cp.start()
        relay_near(1)

        def glu(lhs, gw, uw):
            g = jnp.dot(lhs, gw, preferred_element_type=F32)
            v = jnp.dot(lhs, uw, preferred_element_type=F32)
            return (g * (1.0 / (1.0 + jnp.exp(-g))) * v).astype(BF)

        def glu_unit(lhs, slot, part_, store):
            width, off = (na, 0) if part_ == 0 else (inter - na, na)
            for a in range(0, width, 256):
                b = min(a + 256, width)
                if part_ == 0:
                    gw, uw = wa[2 * slot, :, a:b], wa[2 * slot + 1, :, a:b]
                else:
                    buf = wc1 if slot else wc0
                    gw, uw = buf[0, :, a:b], buf[1, :, a:b]
                store(off + a, off + b, glu(lhs, gw, uw))

        for half, part_ in ((0, 0), (1, 0), (0, 1), (1, 1)):
            for cp in load_shared(half, part_, wc1):
                cp.wait()

            def put(a, b, v):
                act_sh[:, half * inter + a:half * inter + b] = v

            glu_unit(u_all[me], half, part_, put)
            for cp in load_expert(half, half, part_):
                cp.start()
            if (half, part_) == (1, 0):
                relay_near(2)
        for j in range(n_loc + 2):
            load_down(0, j).start()
        relay((6,), dg, (sib,), (0,))
        for k in range(1, n):
            s = lax.rem(me + k, n)
            rcopy(wt_all.at[s], wt_all.at[s], wt_send.at[0], wt_recv.at[s], sib).wait_recv()
        w_all = wt_all[...].reshape(n * n_loc, 128)
        ti = lax.broadcasted_iota(jnp.int32, (128, 128), 0)
        tj = lax.broadcasted_iota(jnp.int32, (128, 128), 1)
        tri = (ti < tj).astype(F32).astype(BF)
        hit = w_all > 0.0
        rank = jnp.dot(hit.astype(F32).astype(BF), tri, preferred_element_type=F32)
        rank_s[...] = jnp.where(hit, rank, -1000.0).reshape(n, n_loc, 128)
        row48 = lax.broadcasted_iota(jnp.int32, (2 * CAP, 256), 0).astype(F32)

        def tables(p, carry):
            for e in range(n_loc):
                rk = jnp.concatenate([rank_s[2 * p, e:e + 1, :], rank_s[2 * p + 1, e:e + 1, :] + float(CAP)], axis=1)
                ww = jnp.concatenate([wt_all[2 * p, e:e + 1, :], wt_all[2 * p + 1, e:e + 1, :]], axis=1)
                sel = row48 == rk
                pm[p, e * 2 * CAP:(e + 1) * 2 * CAP, :] = jnp.where(sel, 1.0, 0.0).astype(BF)
                wsel[e * 2 * CAP:(e + 1) * 2 * CAP, :] = jnp.where(sel, ww, 0.0)
            wt = wsel[...].T
            b1 = wt.astype(BF)
            r1 = wt - b1.astype(F32)
            b2 = r1.astype(BF)
            b3 = (r1 - b2.astype(F32)).astype(BF)
            cm[p, 0:256, :] = b1
            cm[p, 256:512, :] = b2
            cm[p, 512:768, :] = b3
            return carry

        lax.fori_loop(0, 4, tables, 0)

        relay_near(3)
        relay((6,), dg, (sib,), (1, 2))

        def dispatch(p):
            rows = pl.ds(pl.multiple_of(p * 2 * CAP, 16), 2 * CAP)
            for a in range(0, hid, 512):
                uv = u_all[pl.ds(2 * p, 2), :, a:a + 512].reshape(256, 512)
                r = jnp.dot(pm[p], uv, preferred_element_type=F32).astype(BF)
                for e in range(n_loc):
                    xr[e, rows, a:a + 512] = r[e * 2 * CAP:(e + 1) * 2 * CAP]

        arrive(sib)
        dispatch(chip)
        arrive(partner(dev1))
        dispatch(dev1 // 2)
        arrive(partner(dev2))
        dispatch(dev2 // 2)
        relay((6,), dg, (sib,), (3,))
        arrive(partner(dg))
        dispatch(dg // 2)

        def gate_up(k, carry):
            for slot in range(2):
                e = 2 * k + slot

                def put(a, b, v):
                    act[e, :, a:b] = v

                for part_ in range(2):
                    for cp in load_expert(e, slot, part_):
                        cp.wait()
                    glu_unit(xr[e], slot, part_, put)

                    @pl.when(e + 2 < n_loc)
                    def _():
                        for cp in load_expert(e + 2, slot, part_):
                            cp.start()

            for slot in range(2):
                load_routed(0, 2 * k + slot).wait()
            outs = [jnp.dot(act[2 * k + slot], wb[2 * k + slot], preferred_element_type=F32).astype(BF) for slot in range(2)]
            for slot, o in enumerate(outs):
                rows = pl.ds(pl.multiple_of((2 * k + slot) * 2 * CAP, 16), 2 * CAP)
                for p in range(4):
                    orow[p, rows, :] = o[p * 2 * CAP:(p + 1) * 2 * CAP]

            @pl.when(k == n_loc // 2 - 2)
            def _():
                for j in range(n_loc - 2):
                    load_down(1, j).start()

            @pl.when(k == n_loc // 2 - 1)
            def _():
                for j in range(n_loc - 2, n_loc):
                    load_down(1, j).start()
            return carry

        lax.fori_loop(0, n_loc // 2, gate_up, 0)

        for i in range(NSUB):
            for kind, (s, d) in enumerate(((me, dev1), (me, dev2), (me, sib), (dev1, dev2), (dev1, sib), (dev2, sib), (dg, sib))):
                ucopy(kind, s, i, d).wait_send()
        for k in range(1, n):
            wt_copy(k).wait_send()

        def st1(c):
            return rcopy(part.at[lax.rem(c, 2), 1 - core], rx0.at[lax.rem(c, 4)], d_send.at[0, lax.rem(c, 2)], d_recv.at[0, lax.rem(c, 4)], sib)

        def st2(c):
            return rcopy(s1.at[lax.rem(c, 2)], rx1.at[lax.rem(c, 4)], d_send.at[1, lax.rem(c, 2)], d_recv.at[1, lax.rem(c, 4)], dev1)

        def st3(c):
            return rcopy(s2.at[lax.rem(c, 2)], rx2.at[c], d_send.at[2, lax.rem(c, 2)], d_recv.at[2, c], dev2)

        def st4(c):
            return rcopy(s3.at[lax.rem(c, 2)], rx3.at[c], d_send.at[3, lax.rem(c, 2)], d_recv.at[3, c], sib)

        def refill(c, grp):
            @pl.when(c + 1 < nc)
            def _():
                for j in grp:
                    load_down(c + 1, j).start()

        def down(c, grp):
            for j in grp:
                load_down(c, j).wait()
            outs = [jnp.dot(act[e], wb[e], preferred_element_type=F32).astype(BF) for e in grp]
            for e, o in zip(grp, outs):
                for p in range(4):
                    orow[p, e * 2 * CAP:(e + 1) * 2 * CAP, :] = o[p * 2 * CAP:(p + 1) * 2 * CAP]
            refill(c, grp)

        def combine(c):
            sl = lax.rem(c, 2)
            for dy in (1, 0):
                for dx in (1, 0):
                    py = (1 - cy) if dy else cy
                    px = (1 - cx) if dx else cx
                    p = py * 2 + px
                    r3 = jnp.dot(cm[p], orow[p], preferred_element_type=F32)
                    res = r3[0:256] + r3[256:512] + r3[512:768]
                    for h in range(2):
                        a, b = (dx, dy) if h == 0 else (dy, dx)
                        for cc in range(2):
                            part[sl, h, a, b, cc ^ h] = res[cc * 128:(cc + 1) * 128, h * 128:(h + 1) * 128]
            st1(c).start()

        def shared_down(c):
            cols = pl.ds(pl.multiple_of(c * CW, CW), CW)
            grp = (n_loc, n_loc + 1)
            for j in grp:
                load_down(c, j).wait()
            sh = (jnp.dot(act_sh[:, :inter], wb[n_loc], preferred_element_type=F32)
                  + jnp.dot(act_sh[:, inter:], wb[n_loc + 1], preferred_element_type=F32))
            ybase[:, cols] = h1_ref[:, cols].astype(F32) + sh
            refill(c, grp)

        def stage2(k):
            sl = lax.rem(k, 2)
            st1(k).wait_recv()

            @pl.when(k >= 2)
            def _():
                st2(k - 2).wait_send()
            for b in range(2):
                for d in range(2):
                    s1[sl, b, d] = part[sl, core, 1, b, d] + rx0[lax.rem(k, 4), 1, b, d]
            st2(k).start()
            for b in range(2):
                for d in range(2):
                    keep0[sl, b, d] = part[sl, core, 0, b, d] + rx0[lax.rem(k, 4), 0, b, d]
            st1(k).wait_send()

        def stage3(k):
            sl = lax.rem(k, 2)
            st2(k).wait_recv()

            @pl.when(k >= 2)
            def _():
                st3(k - 2).wait_send()
            for d in range(2):
                s2[sl, d] = keep0[sl, 1, d] + rx1[lax.rem(k, 4), 1, d]
            st3(k).start()
            for d in range(2):
                keep1[sl, d] = keep0[sl, 0, d] + rx1[lax.rem(k, 4), 0, d]

        def stage4(k):
            sl = lax.rem(k, 2)
            st3(k).wait_recv()

            @pl.when(k >= 2)
            def _():
                st4(k - 2).wait_send()
            s3[sl] = keep1[sl, 1] + rx2[k, 1]
            st4(k).start()
            keep2[sl] = keep1[sl, 0] + rx2[k, 0]

        def stage5(k):
            mine = pl.ds(pl.multiple_of(k * CW + core * 128, 128), 128)
            other = pl.ds(pl.multiple_of(k * CW + (1 - core) * 128, 128), 128)
            st4(k).wait_recv()
            y_ref[:, mine] = (ybase[:, mine] + keep2[lax.rem(k, 2)]).astype(BF)
            y_ref[:, other] = (ybase[:, other] + rx3[k]).astype(BF)

        def chunk(c, carry):
            live = c < nc
            pl.when(jnp.logical_and(c >= 1, live))(lambda: down(c, (0, 1, 2, 3)))
            pl.when(jnp.logical_and(c >= 1, c < nc + 1))(lambda: stage2(c - 1))
            pl.when(jnp.logical_and(c >= 1, live))(lambda: down(c, (4, 5, 6, 7)))
            pl.when(live)(lambda: combine(c))
            pl.when(live)(lambda: shared_down(c))
            pl.when(jnp.logical_and(c >= 2, c < nc + 2))(lambda: stage3(c - 2))
            pl.when(jnp.logical_and(c >= 3, c < nc + 3))(lambda: stage4(c - 3))
            pl.when(c >= 4)(lambda: stage5(c - 4))
            return carry

        lax.fori_loop(0, nc + 4, chunk, 0)
        for k in (nc - 2, nc - 1):
            st2(k).wait_send()
            st3(k).wait_send()
            st4(k).wait_send()

    pl.run_scoped(
        moe_scope,
        V((n, n_loc, t), F32), V((n_loc * 2 * CAP, 256), F32),
        V((4, n_loc * 2 * CAP, 256), BF), V((4, 768, n_loc * 2 * CAP), BF),
        V((n_loc, 8 * CAP, hid), BF), V((n_loc, 8 * CAP, inter), BF), V((t, 2 * inter), BF),
        V((4, n_loc * 2 * CAP, CW), BF),
        V((2, hid, inter - NA), BF), V((n_loc + 2, inter, CW), BF), V((t, hid), F32),
        V((2, 2, 2, 2, 2, t, 128), F32),
        V((2, 2, 2, t, 128), F32), V((2, 2, 2, t, 128), F32),
        V((2, 2, t, 128), F32), V((2, 2, t, 128), F32), V((2, t, 128), F32), V((2, t, 128), F32))


def copy_kernel(a_ref, b_ref, y_ref, kv_ref):
    y_ref[...] = a_ref[...]
    kv_ref[...] = b_ref[...]


def layer(x, cache, lens, ids, rw, w_q, w_dkv, w_uk, w_uv, w_o, s_gate, s_up, s_down, e_gate, e_up, e_down):
    t, hid = x.shape
    heads, nope, kvl = w_uk.shape
    _, length, kvd = cache.shape
    n_loc = e_gate.shape[0]
    nc = hid // CW
    rot = kvd - kvl
    half = rot // 2
    lane = jnp.arange(128)
    ang = ((lens[:, None] * 128 + lane[None, :]) >> 7).astype(F32) * (ROPE_BASE ** (-2.0 * (lane % half).astype(F32) / rot))[None, :]
    cs4 = jnp.cos(ang)
    sn4 = jnp.sin(ang) * jnp.where(lane % rot < half, -1.0, 1.0)[None, :]
    V = pltpu.VMEM
    D = pltpu.SemaphoreType.DMA
    vm = pl.BlockSpec(memory_space=pltpu.VMEM)
    an = pl.BlockSpec(memory_space=pl.ANY)
    y, kvt = pl.pallas_call(
        layer_kernel,
        out_shape=(jax.ShapeDtypeStruct((t, hid), BF), jax.ShapeDtypeStruct((kvd, t), BF)),
        in_specs=[pl.BlockSpec(memory_space=pltpu.SMEM)] + [vm] * 5 + [an] * 12,
        out_specs=(vm, vm),
        scratch_shapes=[
            V((8, t, hid), BF), V((8 * n_loc, t), F32), V((8, n_loc, t), F32), V((t, hid), BF),
            V((4, hid, NA), BF), V((2, hid, e_gate.shape[2] - NA), BF),
            V((4, 2, 2, 2, t, 128), F32), V((4, 2, 2, t, 128), F32), V((nc, 2, t, 128), F32), V((nc, t, 128), F32),
            D((4,)), D((heads // 4,)), D((RING,)), D((2, 2, 2)), D((n_loc + 2,)), D((8,)), D((8,)),
            D((7, NSUB)), D((8, NSUB)), D((4, 2)), D((4, nc)),
        ],
        compiler_params=pltpu.CompilerParams(collective_id=0, has_side_effects=True, vmem_limit_bytes=67043328),
        name='layer',
    )(lens, ids.T, rw.T, x, cs4, sn4, w_q, w_dkv.T, w_uk, w_uv, w_o, cache.transpose(0, 2, 1),
      s_gate, s_up, s_down, e_gate, e_up, e_down)
    y, kvt = pl.pallas_call(
        copy_kernel,
        out_shape=(jax.ShapeDtypeStruct((t, hid), BF), jax.ShapeDtypeStruct((kvd, t), BF)),
        in_specs=[vm, vm],
        out_specs=(vm, vm),
        name='out',
    )(y, kvt)
    return y, kvt.T


def solution(mesh):
    tok_spec = P(('rep', 'ep'))
    row_spec = P(('rep', 'ep'), None)
    cache_spec = P(('rep', 'ep'), None, None)
    exp_spec = P('ep', None, None)
    in_specs = (row_spec, cache_spec, tok_spec, row_spec, row_spec) + (P(),) * 8 + (exp_spec,) * 3
    return jax.shard_map(layer, mesh=mesh, in_specs=in_specs, out_specs=(row_spec, row_spec), check_vma=False)
```

```python
import jax
import jax.numpy as jnp
import numpy as np
from jax import lax
from jax.experimental import pallas as pl
from jax.experimental.pallas import tpu as pltpu
from jax.sharding import PartitionSpec as P

EPS = 1e-6
ROPE_BASE = 1.0e4
BF = jnp.bfloat16
F32 = jnp.float32
CAP = 24


NB = 16
RING = 2
CW = 256
NA = 768
NSUB = 4
NT = (((1,), (1,)), ((), ()))
SLOT = 2 * CAP
LN = 128
LAST = -1
YES = True


def layer_kernel(lens_ref, lrow_ref, inv_ref, ids_ref, rw_ref, x_ref, wq_h, wdkv_h, wuk_h, wuv_h, wo_h, cache_h,
                 sg, su, sd, eg, eu, ed,
                 y_ref, kvn_ref,
                 u_all, wt_ref, wt_all, h1_ref, wa, wc0, rx0, rx1, rx2, rx3,
                 sem_w, sem_q, sem_c, sem_a, sem_b, wt_send, wt_recv, g_send, g_recv, d_send, d_recv):
    n = 8
    n_loc = eg.shape[0]
    t, hid = x_ref.shape
    inter = eg.shape[2]
    nc = hid // CW
    na = NA
    rsub = t // NSUB
    me = lax.axis_index('ep')
    core = lax.rem(me, 2)
    chip = me // 2
    cx = lax.rem(chip, 2)
    cy = chip // 2
    sib = chip * 2 + 1 - core
    xn_ = (cy * 2 + 1 - cx) * 2 + core
    yn_ = ((1 - cy) * 2 + cx) * 2 + core
    dg = ((1 - cy) * 2 + 1 - cx) * 2 + core
    dev1 = xn_ * (1 - core) + yn_ * core
    dev2 = yn_ * (1 - core) + xn_ * core

    def rcopy(src, dst, ssem, rsem, dev):
        return pltpu.make_async_remote_copy(src_ref=src, dst_ref=dst, send_sem=ssem, recv_sem=rsem,
                                            device_id={'ep': dev}, device_id_type=pl.DeviceIdType.MESH)

    def ucopy(kind, s, i, dev):
        rows = pl.ds(i * rsub, rsub)
        return rcopy(u_all.at[s, rows], u_all.at[s, rows], g_send.at[kind, i], g_recv.at[s, i], dev)

    def arrive(s, subs=range(NSUB)):
        for i in subs:
            ucopy(0, s, i, sib).wait_recv()

    def partner(s):
        return (s // 2) * 2 + 1 - lax.rem(s, 2)

    def wt_copy(k):
        d = lax.rem(me + k, n)
        return rcopy(wt_ref.at[pl.ds(pl.multiple_of(d * n_loc, n_loc), n_loc)], wt_all.at[me],
                     wt_send.at[k], wt_recv.at[me], d)

    def relay(kinds, s, devs, subs):
        for i in subs:
            arrive(s, (i,))
            for kind, dev in zip(kinds, devs):
                cp = ucopy(kind, s, i, dev)
                cp.start()

    def load_unit(srcs, base, slot, part_, wc1):
        if part_ == 0:
            dst, width, off = [wa.at[2 * slot], wa.at[2 * slot + 1]], na, 0
        else:
            buf = wc1 if slot else wc0
            dst, width, off = [buf.at[0], buf.at[1]], inter - na, na
        return [pltpu.make_async_copy(src.at[:, pl.ds(base + off, width)], d, sem_a.at[part_, slot, i])
                for i, (src, d) in enumerate(zip(srcs, dst))]

    def load_shared(half, part_, wc1=None):
        return load_unit((sg, su), half * inter, half, part_, wc1)

    def relay_near(i):
        relay((3, 4), dev1, (dev2, sib), (i,))
        relay((5,), dev2, (sib,), (i,))

    na_blk = t * 3 // 4 // NB

    def attn_scope(wdkv, wuk, wuv, wo, cbuf, qs, kvs, os, oc):
        heads, nope, kvl = wuk.shape
        kvd = cbuf.shape[2]
        rot = kvd - kvl
        qkd = nope + rot
        length = cbuf.shape[3]
        vh = wuv.shape[2]
        nblk = t // NB
        qw = 4 * qkd
        nq = heads // 4
        scale = qkd ** -0.5

        cp_dkv = pltpu.make_async_copy(wdkv_h, wdkv, sem_w.at[0])
        cp_uk = pltpu.make_async_copy(wuk_h, wuk, sem_w.at[1])
        cp_uv = pltpu.make_async_copy(wuv_h, wuv, sem_w.at[2])
        cp_o = pltpu.make_async_copy(wo_h, wo, sem_w.at[3])
        cp_q = [pltpu.make_async_copy(wq_h.at[:, i * qw:(i + 1) * qw], wa.at[i], sem_q.at[i]) for i in range(nq)]

        def load(b):
            sl = lax.rem(b, RING)
            return pltpu.make_async_copy(cache_h.at[pl.ds(b * NB, NB)], cbuf.at[sl], sem_c.at[sl])

        cp_dkv.start()
        cp_q[0].start()
        cp_uk.start()
        for cp in cp_q[1:]:
            cp.start()
        for b in range(RING):
            load(b).start()
        cp_uv.start()
        cp_o.start()

        barrier = pltpu.get_barrier_semaphore()
        for k in range(1, n):
            pl.semaphore_signal(barrier, inc=1, device_id={'ep': lax.rem(me + k, n)}, device_id_type=pl.DeviceIdType.MESH)
        pl.semaphore_wait(barrier, n - 1)

        ex = lax.broadcasted_iota(jnp.int32, wt_ref.shape, 0)
        wt = jnp.zeros(wt_ref.shape, F32)
        for k in range(ids_ref.shape[0]):
            wt = wt + jnp.where(ids_ref[k:k + 1, :] == ex, rw_ref[k:k + 1, :], 0.0)
        wt_ref[...] = wt
        wt_all[me] = wt_ref[pl.ds(pl.multiple_of(me * n_loc, n_loc), n_loc), :]
        lane = lax.broadcasted_iota(jnp.int32, (t, 128), 1)
        ang = jnp.broadcast_to(lrow_ref[...].astype(F32), (128, t)).T * inv_ref[...]
        cs = jnp.cos(ang)
        sn = jnp.where(lax.rem(lane, rot) < rot // 2, -jnp.sin(ang), jnp.sin(ang))
        low = lax.rem(lane, rot) < rot // 2

        def rope2(v):
            sw = jnp.where(low, pltpu.roll(v, 128 - rot // 2, 1), pltpu.roll(v, rot // 2, 1))
            return v * cs + sw * sn

        xf = x_ref[...].astype(F32)
        xn = (xf * lax.rsqrt(jnp.mean(xf * xf, axis=LAST, keepdims=YES) + EPS)).astype(BF)

        cp_dkv.wait()
        kv = lax.dot_general(xn, wdkv[...], NT, preferred_element_type=F32)
        kl = kv[:, :kvl]
        kl = (kl * lax.rsqrt(jnp.mean(kl * kl, axis=LAST, keepdims=YES) + EPS)).astype(BF)
        kr = kv[:, kvl:kvd]
        kr = rope2(jnp.concatenate([kr, kr], axis=1)).astype(BF)
        kvs[:, :kvl] = kl.astype(F32)
        kvs[:, kvl:kvl + LN] = jnp.where(lane < rot, kr.astype(F32), 0.0)
        kvn_ref[...] = kvs[...].T[:kvd].astype(BF)

        for k in range(1, n):
            wt_copy(k).start()

        for i in range(nq):
            cp_q[i].wait()
            qc = jnp.dot(xn, wa[i], preferred_element_type=F32).astype(BF).astype(F32)
            if i == 0:
                cp_uk.wait()
            for j in range(2):
                o0 = j * 2 * qkd
                h = i * 4 + j * 2
                n0 = qc[:, o0:o0 + nope].astype(BF)
                n1 = qc[:, o0 + qkd:o0 + qkd + nope].astype(BF)
                r = jnp.concatenate([qc[:, o0 + nope:o0 + qkd], qc[:, o0 + qkd + nope:o0 + 2 * qkd]], axis=1)
                r = rope2(r).astype(BF).astype(F32)
                qs[:, h, :kvl] = jnp.dot(n0, wuk[h], preferred_element_type=F32).astype(BF).astype(F32)
                qs[:, h + 1, :kvl] = jnp.dot(n1, wuk[h + 1], preferred_element_type=F32).astype(BF).astype(F32)
                qs[:, h, kvl:kvl + LN] = jnp.where(lane < rot, r, 0.0)
                qs[:, h + 1, kvl:kvl + LN] = jnp.where(lane < rot, pltpu.roll(r, rot, 1), 0.0)

        pos = lax.broadcasted_iota(jnp.int32, (heads, length), 1)

        def block(b, carry):
            sl = lax.rem(b, RING)
            load(b).wait()
            ss = []
            sns = []
            for i in range(NB):
                qf = qs[b * NB + i]
                qb = qf[:, 0:kvd].astype(BF)
                ss.append(jnp.dot(qb, cbuf[sl, i], preferred_element_type=F32))
                sns.append(jnp.sum(qf * kvs[pl.ds(b * NB + i, 1), :], axis=LAST, keepdims=YES) * scale)
            for i in range(NB):
                s = jnp.where(pos < lens_ref[b * NB + i], ss[i] * scale, -jnp.inf)
                mx = jnp.maximum(jnp.max(s, axis=LAST, keepdims=YES), sns[i])
                e = jnp.exp(s - mx)
                en = jnp.exp(sns[i] - mx)
                den = jnp.sum(e, axis=LAST, keepdims=YES) + en
                p = (e / den).astype(BF)
                pn = (en / den).astype(BF).astype(F32)
                o = lax.dot_general(p, cbuf[sl, i, :kvl, :], NT, preferred_element_type=F32)
                os[:, lax.rem(b, na_blk) * NB + i, :] = o + pn * kvs[pl.ds(b * NB + i, 1), :kvl]

            @pl.when(b + RING < nblk)
            def _():
                load(b + RING).start()

            for j, cp in enumerate(load_shared(0, 0) + load_shared(1, 0) + load_shared(0, 1)):
                pl.when(b == j + 2)(cp.start)
            return carry

        for half in range(2):
            lax.fori_loop((0, na_blk)[half], (na_blk, nblk)[half], block, 0)
            if half == 0:
                cp_uv.wait()
                cp_o.wait()
            else:
                relay_near(0)
            rows = slice((0, na_blk * NB)[half], (na_blk * NB, t)[half])
            nh = rows.stop - rows.start
            for h in range(heads):
                oc[:nh, h * vh:(h + 1) * vh] = jnp.dot(os[h, :nh].astype(BF), wuv[h], preferred_element_type=F32).astype(BF)
            ssq = jnp.zeros((nh, 1), F32)
            for a in range(0, hid, 512):
                h1 = (x_ref[rows, a:a + 512].astype(F32)
                      + jnp.dot(oc[:nh], wo[:, a:a + 512], preferred_element_type=F32)).astype(BF)
                h1_ref[rows, a:a + 512] = h1
                hf = h1.astype(F32)
                ssq = ssq + jnp.sum(hf * hf, axis=LAST, keepdims=YES)
            inv = lax.rsqrt(ssq * (1.0 / hid) + EPS)
            u_all[me, rows, :] = (h1_ref[rows, :].astype(F32) * inv).astype(BF)
            for i in range(rows.start // rsub, rows.stop // rsub):
                for kind, d in enumerate((dev1, dev2, sib)):
                    cp = ucopy(kind, me, i, d)
                    cp.start()

    heads, nope, kvl = wuk_h.shape
    vh = wuv_h.shape[2]
    _, kvd, length = cache_h.shape
    V = pltpu.VMEM
    pl.run_scoped(
        attn_scope,
        V((kvd, hid), BF), V((heads, nope, kvl), BF),
        V((heads, kvl, vh), BF), V((heads * vh, hid), BF), V((RING, NB, kvd, length), BF),
        V((t, heads, kvl + 128), F32), V((t, kvl + 128), F32), V((heads, na_blk * NB, kvl), F32), V((na_blk * NB, heads * vh), BF))

    def moe_scope(rank_s, wsel, pm, cm, xr, act, act_sh, orow, wc1, wb, ybase,
                  part, s1, keep0, s2, keep1, s3, keep2):
        def load_expert(e, slot, part_):
            return load_unit((eg.at[e], eu.at[e]), 0, slot, part_, wc1)

        def load_routed(c, e):
            cols = pl.ds(pl.multiple_of(c * CW, CW), CW)
            return pltpu.make_async_copy(ed.at[e, :, cols], wb.at[e], sem_b.at[e])

        def load_down(c, j):
            cols = pl.ds(pl.multiple_of(c * CW, CW), CW)
            if j < n_loc:
                src = ed.at[j, :, cols]
            else:
                src = sd.at[pl.ds((j - n_loc) * inter, inter), cols]
            return pltpu.make_async_copy(src, wb.at[j], sem_b.at[j])

        for cp in load_shared(1, 1, wc1):
            cp.start()
        relay_near(1)

        def act_fn(g, v):
            return (g * (1.0 / (1.0 + jnp.exp(-g))) * v).astype(BF)

        def glu(lhs, gw, uw):
            g = jnp.dot(lhs, gw, preferred_element_type=F32)
            v = jnp.dot(lhs, uw, preferred_element_type=F32)
            return act_fn(g, v)

        def glu_unit(lhs, slot, part_, store):
            width, off = (na, 0) if part_ == 0 else (inter - na, na)
            for a in range(0, width, 256):
                b = min(a + 256, width)
                if part_ == 0:
                    gw, uw = wa[2 * slot, :, a:b], wa[2 * slot + 1, :, a:b]
                else:
                    buf = wc1 if slot else wc0
                    gw, uw = buf[0, :, a:b], buf[1, :, a:b]
                if b - a == 128:
                    gv = jnp.dot(lhs, jnp.concatenate([gw, uw], axis=1), preferred_element_type=F32)
                    store(off + a, off + b, act_fn(gv[:, :LN], gv[:, LN:2 * LN]))
                else:
                    store(off + a, off + b, glu(lhs, gw, uw))

        for half, part_ in ((0, 0), (1, 0), (0, 1), (1, 1)):
            for cp in load_shared(half, part_, wc1):
                cp.wait()

            def put(a, b, v):
                act_sh[:, half * inter + a:half * inter + b] = v

            glu_unit(u_all[me], half, part_, put)
            for cp in load_expert(half, half, part_):
                cp.start()
            if (half, part_) == (1, 0):
                relay_near(2)
        for j in range(n_loc + 2):
            load_down(0, j).start()
        relay((6,), dg, (sib,), (0,))
        for k in range(1, n):
            s = lax.rem(me + k, n)
            rcopy(wt_all.at[s], wt_all.at[s], wt_send.at[0], wt_recv.at[s], sib).wait_recv()
        w_all = wt_all[...].reshape(n * n_loc, 128)
        ti = lax.broadcasted_iota(jnp.int32, (128, 128), 0)
        tj = lax.broadcasted_iota(jnp.int32, (128, 128), 1)
        tri = (ti < tj).astype(F32).astype(BF)
        hit = w_all > 0.0
        rank = jnp.dot(hit.astype(F32).astype(BF), tri, preferred_element_type=F32)
        rank_s[...] = jnp.where(hit, rank, -1000.0).reshape(n, n_loc, 128)
        row48 = lax.broadcasted_iota(jnp.int32, (SLOT, 256), 0).astype(F32)

        def tables(p, carry):
            for e in range(n_loc):
                rk = jnp.concatenate([rank_s[2 * p, e:e + 1, :], rank_s[2 * p + 1, e:e + 1, :] + float(CAP)], axis=1)
                ww = jnp.concatenate([wt_all[2 * p, e:e + 1, :], wt_all[2 * p + 1, e:e + 1, :]], axis=1)
                sel = row48 == rk
                pm[p, e * SLOT:(e + 1) * SLOT, :] = jnp.where(sel, 1.0, 0.0).astype(BF)
                wsel[e * SLOT:(e + 1) * SLOT, :] = jnp.where(sel, ww, 0.0)
            wt = wsel[...].T
            b1 = wt.astype(BF)
            r1 = wt - b1.astype(F32)
            b2 = r1.astype(BF)
            b3 = (r1 - b2.astype(F32)).astype(BF)
            th = t // 2
            for i, b in enumerate((b1, b2, b3)):
                for sub in range(2):
                    for cc in range(2):
                        r0 = ((sub * 3 + i) * 2 + cc) * th
                        cm[p, r0:r0 + th, :] = b[cc * t + sub * th:cc * t + (sub + 1) * th]
            return carry

        lax.fori_loop(0, 4, tables, 0)

        relay_near(3)
        relay((6,), dg, (sib,), (1, 2))

        def dispatch(p):
            rows = pl.ds(pl.multiple_of(p * SLOT, 16), SLOT)
            for a in range(0, hid, 512):
                uv = u_all[pl.ds(2 * p, 2), :, a:a + 512].reshape(256, 512)
                r = jnp.dot(pm[p], uv, preferred_element_type=F32).astype(BF)
                for e in range(n_loc):
                    xr[e, rows, a:a + 512] = r[e * SLOT:(e + 1) * SLOT]

        arrive(sib)
        dispatch(chip)
        arrive(partner(dev1))
        dispatch(dev1 // 2)
        arrive(partner(dev2))
        dispatch(dev2 // 2)
        relay((6,), dg, (sib,), (3,))
        arrive(partner(dg))
        dispatch(dg // 2)

        def gate_up(k, carry):
            for slot in range(2):
                e = 2 * k + slot

                def put(a, b, v):
                    act[e, :, a:b] = v

                for part_ in range(2):
                    for cp in load_expert(e, slot, part_):
                        cp.wait()
                    glu_unit(xr[e], slot, part_, put)

                    @pl.when(e + 2 < n_loc)
                    def _():
                        for cp in load_expert(e + 2, slot, part_):
                            cp.start()

            for slot in range(2):
                load_routed(0, 2 * k + slot).wait()
            outs = [jnp.dot(act[2 * k + slot], wb[2 * k + slot], preferred_element_type=F32).astype(BF) for slot in range(2)]
            for slot, o in enumerate(outs):
                rows = pl.ds(pl.multiple_of((2 * k + slot) * SLOT, 16), SLOT)
                for p in range(4):
                    orow[p, rows, :] = o[p * SLOT:(p + 1) * SLOT]

            @pl.when(k == n_loc // 2 - 2)
            def _():
                for j in range(n_loc - 2):
                    load_down(1, j).start()

            @pl.when(k == n_loc // 2 - 1)
            def _():
                for j in range(n_loc - 2, n_loc):
                    load_down(1, j).start()
            return carry

        lax.fori_loop(0, n_loc // 2, gate_up, 0)

        for i in range(NSUB):
            for kind, (s, d) in enumerate(((me, dev1), (me, dev2), (me, sib), (dev1, dev2), (dev1, sib), (dev2, sib), (dg, sib))):
                ucopy(kind, s, i, d).wait_send()
        for k in range(1, n):
            wt_copy(k).wait_send()

        th = t // 2

        def st1(q):
            return rcopy(part.at[lax.rem(q, 2), 1 - core], rx0.at[lax.rem(q, 4)], d_send.at[0, lax.rem(q, 4)], d_recv.at[0, lax.rem(q, 4)], sib)

        def st2(q):
            return rcopy(s1.at[lax.rem(q, 4)], rx1.at[lax.rem(q, 8)], d_send.at[1, lax.rem(q, 4)], d_recv.at[1, lax.rem(q, 8)], dev1)

        def st3(q):
            return rcopy(s2.at[lax.rem(q, 4)], rx2.at[q], d_send.at[2, lax.rem(q, 4)], d_recv.at[2, q], dev2)

        def st4(q):
            return rcopy(s3.at[lax.rem(q, 4)], rx3.at[q], d_send.at[3, lax.rem(q, 4)], d_recv.at[3, q], sib)

        def refill(c, grp):
            @pl.when(c + 1 < nc)
            def _():
                for j in grp:
                    load_down(c + 1, j).start()

        def down(c, grp):
            for j in grp:
                load_down(c, j).wait()
            outs = [jnp.dot(act[e], wb[e], preferred_element_type=F32).astype(BF) for e in grp]
            for e, o in zip(grp, outs):
                for p in range(4):
                    orow[p, e * SLOT:(e + 1) * SLOT, :] = o[p * SLOT:(p + 1) * SLOT]
            refill(c, grp)

        def combine(q, sub):
            for dy in (1, 0):
                for dx in (1, 0):
                    py = (1 - cy) if dy else cy
                    px = (1 - cx) if dx else cx
                    p = py * 2 + px
                    r3 = jnp.dot(cm[p, sub * 6 * th:(sub + 1) * 6 * th, :], orow[p], preferred_element_type=F32)
                    res = r3[:t] + r3[t:2 * t] + r3[2 * t:3 * t]
                    for h in range(2):
                        a, b = (dx, dy) if h == 0 else (dy, dx)
                        for cc in range(2):
                            part[sub, h, a, b, cc ^ h] = res[cc * th:(cc + 1) * th, h * 128:(h + 1) * 128]
            st1(q).start()

        def shared_down(c):
            cols = pl.ds(pl.multiple_of(c * CW, CW), CW)
            grp = (n_loc, n_loc + 1)
            for j in grp:
                load_down(c, j).wait()
            sh = (jnp.dot(act_sh[:, :inter], wb[n_loc], preferred_element_type=F32)
                  + jnp.dot(act_sh[:, inter:], wb[n_loc + 1], preferred_element_type=F32))
            ybase[:, cols] = h1_ref[:, cols].astype(F32) + sh
            refill(c, grp)

        def stage2(k):
            sl = lax.rem(k, 2)
            s4 = lax.rem(k, 4)
            st1(k).wait_recv()

            @pl.when(k >= 4)
            def _():
                st2(k - 4).wait_send()
            for b in range(2):
                for d in range(2):
                    s1[s4, b, d] = part[sl, core, 1, b, d] + rx0[s4, 1, b, d]
            st2(k).start()
            for b in range(2):
                for d in range(2):
                    keep0[s4, b, d] = part[sl, core, 0, b, d] + rx0[s4, 0, b, d]
            st1(k).wait_send()

        def stage3(k):
            s4 = lax.rem(k, 4)
            st2(k).wait_recv()

            @pl.when(k >= 4)
            def _():
                st3(k - 4).wait_send()
            for d in range(2):
                s2[s4, d] = keep0[s4, 1, d] + rx1[lax.rem(k, 8), 1, d]
            st3(k).start()
            for d in range(2):
                keep1[s4, d] = keep0[s4, 0, d] + rx1[lax.rem(k, 8), 0, d]

        def stage4(k):
            s4 = lax.rem(k, 4)
            st3(k).wait_recv()

            @pl.when(k >= 4)
            def _():
                st4(k - 4).wait_send()
            s3[s4] = keep1[s4, 1] + rx2[k, 1]
            st4(k).start()
            keep2[s4] = keep1[s4, 0] + rx2[k, 0]

        def stage5(k):
            c = k // 2
            mine = pl.ds(pl.multiple_of(c * CW + core * 128, 128), 128)
            other = pl.ds(pl.multiple_of(c * CW + (1 - core) * 128, 128), 128)
            rows = pl.ds(pl.multiple_of(lax.rem(k, 2) * th, th), th)
            st4(k).wait_recv()
            y_ref[rows, mine] = (ybase[rows, mine] + keep2[lax.rem(k, 4)]).astype(BF)
            y_ref[rows, other] = (ybase[rows, other] + rx3[k]).astype(BF)

        nq2 = 2 * nc

        def pipe(lag, fn, q):
            pl.when(jnp.logical_and(q >= lag, q < nq2 + lag))(lambda: fn(q - lag))

        def chunk(c, carry):
            live = c < nc
            q = 2 * c
            pl.when(jnp.logical_and(c >= 1, live))(lambda: down(c, (0, 1, 2, 3)))
            pipe(1, stage2, q)
            pl.when(jnp.logical_and(c >= 1, live))(lambda: down(c, (4, 5, 6, 7)))
            pl.when(live)(lambda: combine(q, 0))
            pipe(3, stage3, q)
            pipe(5, stage4, q)
            pipe(6, stage5, q)
            q = 2 * c + 1
            pl.when(live)(lambda: combine(q, 1))
            pipe(1, stage2, q)
            pl.when(live)(lambda: shared_down(c))
            pipe(3, stage3, q)
            pipe(5, stage4, q)
            pipe(6, stage5, q)
            return carry

        lax.fori_loop(0, nc + 3, chunk, 0)
        for k in range(nq2 - 4, nq2):
            st2(k).wait_send()
            st3(k).wait_send()
            st4(k).wait_send()

    pl.run_scoped(
        moe_scope,
        V((n, n_loc, t), F32), V((n_loc * SLOT, 256), F32),
        V((4, n_loc * SLOT, 256), BF), V((4, 768, n_loc * SLOT), BF),
        V((n_loc, 8 * CAP, hid), BF), V((n_loc, 8 * CAP, inter), BF), V((t, 2 * inter), BF),
        V((4, n_loc * SLOT, CW), BF),
        V((2, hid, inter - NA), BF), V((n_loc + 2, inter, CW), BF), V((t, hid), F32),
        V((2, 2, 2, 2, 2, t // 2, LN), F32),
        V((4, 2, 2, t // 2, LN), F32), V((4, 2, 2, t // 2, LN), F32),
        V((4, 2, t // 2, LN), F32), V((4, 2, t // 2, LN), F32), V((4, t // 2, LN), F32), V((4, t // 2, LN), F32))


def copy_kernel(a_ref, b_ref, y_ref, kv_ref):
    y_ref[...] = a_ref[...]
    kv_ref[...] = b_ref[...]


def layer(x, cache, lens, ids, rw, w_q, w_dkv, w_uk, w_uv, w_o, s_gate, s_up, s_down, e_gate, e_up, e_down):
    t, hid = x.shape
    heads, nope, kvl = w_uk.shape
    _, length, kvd = cache.shape
    n_loc = e_gate.shape[0]
    nc = hid // CW
    rot = kvd - kvl
    half = rot // 2
    inv = np.tile(ROPE_BASE ** (-2.0 * np.arange(half) / rot), 128 // half)[None, :].astype(np.float32)
    V = pltpu.VMEM
    D = pltpu.SemaphoreType.DMA
    vm = pl.BlockSpec(memory_space=pltpu.VMEM)
    an = pl.BlockSpec(memory_space=pl.ANY)
    y, kvt = pl.pallas_call(
        layer_kernel,
        out_shape=(jax.ShapeDtypeStruct((t, hid), BF), jax.ShapeDtypeStruct((kvd, t), BF)),
        in_specs=[pl.BlockSpec(memory_space=pltpu.SMEM)] + [vm] * 5 + [an] * 12,
        out_specs=(vm, vm),
        scratch_shapes=[
            V((8, t, hid), BF), V((8 * n_loc, t), F32), V((8, n_loc, t), F32), V((t, hid), BF),
            V((4, hid, NA), BF), V((2, hid, e_gate.shape[2] - NA), BF),
            V((4, 2, 2, 2, t // 2, LN), F32), V((8, 2, 2, t // 2, LN), F32),
            V((2 * nc, 2, t // 2, LN), F32), V((2 * nc, t // 2, LN), F32),
            D((4,)), D((heads // 4,)), D((RING,)), D((2, 2, 2)), D((n_loc + 2,)), D((8,)), D((8,)),
            D((7, NSUB)), D((8, NSUB)), D((4, 4)), D((4, 2 * nc)),
        ],
        compiler_params=pltpu.CompilerParams(collective_id=0, has_side_effects=True, vmem_limit_bytes=67043328),
        name='layer',
    )(lens, lens.reshape(1, t), jnp.asarray(inv), ids.T, rw.T, x, w_q, w_dkv.T, w_uk, w_uv, w_o, cache.transpose(0, 2, 1),
      s_gate, s_up, s_down, e_gate, e_up, e_down)
    y, kvt = pl.pallas_call(
        copy_kernel,
        out_shape=(jax.ShapeDtypeStruct((t, hid), BF), jax.ShapeDtypeStruct((kvd, t), BF)),
        in_specs=[vm, vm],
        out_specs=(vm, vm),
        name='out',
    )(y, kvt)
    return y, kvt.T


def solution(mesh):
    tok_spec = P(('rep', 'ep'))
    row_spec = P(('rep', 'ep'), None)
    cache_spec = P(('rep', 'ep'), None, None)
    exp_spec = P('ep', None, None)
    in_specs = (row_spec, cache_spec, tok_spec, row_spec, row_spec) + (P(),) * 8 + (exp_spec,) * 3
    return jax.shard_map(layer, mesh=mesh, in_specs=in_specs, out_specs=(row_spec, row_spec), check_vma=False)
```
